256 devices in a mesh: expert: 8 (over z), tensor: 4 (over y), dp: 8 (over x, core).
Axes of the slice: x: 4, y: 4, z: 8, core: 2. Of those that a mesh axis runs over, the one named last changes fastest.
Arguments:
- hidden_in: bfloat16 [8, 512, 4096], P('dp', 'expert'), may hold values from -64 to 64
- expert_ids: int32 [8, 512, 2], P('dp', 'expert'), may hold values from 0 to 7, all different within a row; in each aligned block of 64 rows (0 to 63, 64 to 127, ..., all dimensions but the last counted through in order) at most 18 rows name the same one
- ffn_gain: float32 [4096], replicated, may hold values from 0.5 to 1.5
- w_router: bfloat16 [4096, 8], replicated, may hold values from -0.09375 to 0.09375
- w_gate: bfloat16 [8, 4096, 14336], P('expert', None, ('tensor', 'dp')), may hold values from -0.09375 to 0.09375
- w_up: bfloat16 [8, 4096, 14336], P('expert', None, ('tensor', 'dp')), may hold values from -0.09375 to 0.09375
- w_down: bfloat16 [8, 14336, 4096], P('expert', ('tensor', 'dp')), may hold values from -0.046875 to 0.046875
Outputs:
- hidden_out: bfloat16 [8, 512, 4096], P('dp', 'expert', 'tensor')
- layer_score: float32 [], replicated
The draws below stay inside these ranges and needn't reach their ends.
Inputs may be any that keep to these rules, and one draw needn't show every extreme that they name: `expert_ids`: among the 64 tokens of one device (aligned blocks of the flattened sequence and position order), no expert is chosen by more than 18 of them; a token's two experts differ.
All inputs are finite; a program needn't handle non-finite values.
Results may differ from the reference program's by a relative error of at most 0.0027.
Values may be sent and summed in bfloat16 or wider, within the bound.
A program may use at most 128 MiB of HBM per device.

```python
import math
import jax
import jax.numpy as jnp
import numpy as np
from jax import lax

D = 4096
FF = 14336
TOP = 2
LEN = 512
EXPERTS = 8
SEQS = 8
TOK_DEV = 64
CAP = 18


def draw_hidden_in(key, part):
    key_base, key_jitter, key_columns = jax.random.split(key, 3)
    token_count = SEQS * LEN
    flat_index = jnp.arange(token_count, dtype=jnp.int32)
    position_frac = (flat_index % LEN).astype(jnp.float32) / (LEN - 1)
    sequence_frac = (flat_index // LEN).astype(jnp.float32) / max(SEQS - 1, 1)
    place = 0.75 * position_frac + 0.25 * sequence_frac
    jitter = jax.random.uniform(key_jitter, (token_count,), jnp.float32, 0.0, 1.0)
    row_scale = jnp.exp(jnp.log(0.5) + jnp.log(8.0) * place + 0.4 * (jitter - 0.5))
    column_scale = jnp.exp(jax.random.uniform(key_columns, (D,), jnp.float32, jnp.log(0.3), jnp.log(3.0)))
    base_draw = jax.random.normal(key_base, (token_count, D), jnp.float32)
    values = jnp.clip(base_draw * row_scale[:, None] * column_scale[None, :], -64.0, 64.0)
    return values.reshape(SEQS, LEN, D).astype(jnp.bfloat16)


def level_of(key, shape, pieces, smallest, top_value):
    factor_of, own = 1.0, jax.random.fold_in(key, 6)
    for axis_at, parts in pieces:
        steps = jnp.exp(jax.random.uniform(jax.random.fold_in(own, axis_at), (parts,), jnp.float32, smallest / len(pieces), top_value / len(pieces)))
        factor_of = factor_of * jnp.repeat(steps, shape[axis_at] // parts).reshape([-1 if axis == axis_at else 1 for axis in range(len(shape))])
    return factor_of


def deal_out(own_key, own, number, rows, number_of, top, reach, slope):
    sequence = jax.random.permutation(own_key, number_of)
    crowded, usual = portions_of(number_of, rows * top, reach, slope, True), portions_of(number_of, rows * top, reach, slope, False)
    places = jnp.arange(number_of)

    def named(lengths, rotation):
        used = int((lengths > 0).sum())
        fixed = max(1, used // 4)
        moved = fixed + (places - fixed + rotation * (used - fixed)) % max(1, number_of - fixed)
        return jnp.zeros((number_of,), jnp.int32).at[sequence[jnp.where(places < fixed, places, moved)]].set(jnp.asarray(lengths, jnp.int32))

    lengths = jnp.where(number % 4 == 0, named(crowded, number // 4), named(usual, number - number // 4 - 1))
    mixed = jax.random.permutation(jax.random.fold_in(own, 3), number_of)
    source_of, sink = mixed[0:number_of // 2 * 2:2], mixed[1:number_of // 2 * 2:2]
    room = jnp.minimum(lengths[source_of] - 1, reach - lengths[sink]) // 2
    room = jnp.where((source_of == sequence[0]) | (sink == sequence[0]) | (lengths[sink] == 0), 0, jnp.maximum(room, 0))
    moved = jax.random.randint(jax.random.fold_in(own, 4), (number_of // 2,), 0, 1 << 20) % (room + 1)
    lengths = lengths.at[source_of].add(-moved).at[sink].add(moved)
    members = jnp.searchsorted(jnp.cumsum(lengths), jnp.arange(rows * top), side="right").astype(jnp.int32)
    grid = members.reshape(top, rows).T
    grid = grid[jax.random.permutation(jax.random.fold_in(own, 1), rows)]
    rotation = jax.random.randint(jax.random.fold_in(own, 2), (rows, 1), 0, top)
    return jnp.take_along_axis(grid, (jnp.arange(top)[None, :] + rotation) % top, axis=1)


def portions_of(number_of, total, limit, slope, full):
    portions = [(1 << 20) // math.isqrt(grade ** slope) + 1 for grade in range(1, number_of + 1)]
    largest = limit if full else min(limit, max(-(-total // number_of), total * portions[0] // sum(portions)))
    least = 1 if total - largest >= number_of - 1 else 0
    counts, spare = [largest] + [least] * (number_of - 1), total - largest - least * (number_of - 1)
    while spare > 0:
        movable = [i for i in range(1, number_of) if counts[i] < largest] or [i for i in range(1, number_of) if counts[i] < limit]
        whole, left = sum([portions[i] for i in movable]), spare
        for i in movable:
            more = min(limit - counts[i], max(1, left * portions[i] // whole), spare)
            counts[i] = counts[i] + more
            spare = spare - more
    return np.array(counts)


def gaussian(rng, dims, scale, bound, shards=(), kind=jnp.bfloat16):
    entries = scale * jax.random.normal(rng, dims, jnp.float32)
    if shards:
        entries = entries * level_of(rng, dims, shards, -0.22, 0.18)
    return jnp.clip(entries, -bound, bound).astype(kind)


def setup_inputs(seed: int = 0) -> dict:
    streams_of = jax.random.split(jax.random.key(seed), 8)
    hidden_in = draw_hidden_in(jax.random.fold_in(streams_of[7], 71), 0)
    expert_ids_keys = jax.random.split(jax.random.fold_in(streams_of[1], 1), SEQS * LEN // TOK_DEV)
    expert_ids_turns = jax.random.permutation(jax.random.fold_in(streams_of[1], 3), SEQS * LEN // TOK_DEV)
    expert_ids = jax.vmap(lambda own, number: deal_out(jax.random.fold_in(streams_of[1], 2), own, number, TOK_DEV, EXPERTS, TOP, CAP, 1))(expert_ids_keys, expert_ids_turns).reshape((SEQS, LEN, TOP))
    ffn_gain = jnp.clip(1.0 + 0.1 * jax.random.normal(streams_of[2], (D,), jnp.float32), 0.5, 1.5)
    w_router = gaussian(streams_of[3], (D, EXPERTS), D ** -0.5, 0.09375)
    w_gate = gaussian(streams_of[4], (EXPERTS, D, FF), D ** -0.5, 0.09375, ((0, 8), (2, 32)))
    w_up = gaussian(streams_of[5], (EXPERTS, D, FF), D ** -0.5, 0.09375, ((0, 8), (2, 32)))
    w_down = gaussian(streams_of[6], (EXPERTS, FF, D), FF ** -0.5, 0.046875, ((0, 8), (1, 32)))
    return dict(hidden_in=hidden_in, expert_ids=expert_ids, ffn_gain=ffn_gain, w_router=w_router, w_gate=w_gate, w_up=w_up, w_down=w_down)


EPS_NORM = 1e-05
EPS_COS = 1e-06

def slot_positions(flat_ids):
    pair_count = flat_ids.shape[0]
    onehot = (flat_ids[:, None] == jnp.arange(EXPERTS, dtype=jnp.int32)[None, :]).astype(jnp.int32)
    positions = jnp.arange(pair_count, dtype=jnp.int32)
    earlier = (positions[None, :] < positions[:, None]).astype(jnp.int32)
    before = lax.optimization_barrier(jnp.sum(earlier[:, :, None] * onehot[None, :, :], axis=1))
    return lax.optimization_barrier(jnp.sum(before * onehot, axis=1)).astype(jnp.int32)

def reference(hidden_in, expert_ids, ffn_gain, w_router, w_gate, w_up, w_down):
    token_count = SEQS * LEN
    blocks = token_count // TOK_DEV
    token_rows = hidden_in.reshape(token_count, D).astype(jnp.float32)
    inverse_rms = lax.rsqrt(lax.optimization_barrier(jnp.mean(token_rows * token_rows, axis=1, keepdims=True)) + EPS_NORM)
    normed = (token_rows * inverse_rms * ffn_gain[None, :]).astype(jnp.bfloat16)
    logits = jnp.dot(normed, w_router, preferred_element_type=jnp.float32)
    chosen = expert_ids.reshape(token_count, TOP).astype(jnp.int32)
    selector = (chosen[:, :, None] == jnp.arange(EXPERTS, dtype=jnp.int32)[None, None, :]).astype(jnp.float32)
    picked = lax.optimization_barrier(jnp.sum(selector * logits[:, None, :], axis=2))
    spread = picked[:, 0] - picked[:, 1]
    gate_values = jnp.stack([jax.nn.sigmoid(spread), jax.nn.sigmoid(-spread)], axis=1)
    slot_index = lax.map(slot_positions, chosen.reshape(blocks, TOK_DEV * TOP)).reshape(token_count, TOP)
    block_of = (jnp.arange(token_count, dtype=jnp.int32) // TOK_DEV)[:, None]
    places = (chosen * (blocks * CAP) + block_of * CAP + slot_index).reshape(-1).astype(jnp.int32)
    sources = jnp.broadcast_to(jnp.arange(token_count, dtype=jnp.int32)[:, None], (token_count, TOP)).reshape(-1)
    slot_table = jnp.full((EXPERTS * blocks * CAP,), token_count, dtype=jnp.int32).at[places].set(sources)
    slot_table = slot_table.reshape(EXPERTS, blocks * CAP)
    padded = jnp.concatenate([normed, jnp.zeros((1, D), jnp.bfloat16)], axis=0)

    def run_expert(operands):
        table_row, gate_matrix, up_matrix, down_matrix = operands
        inputs = padded[table_row]
        gate_term = jnp.dot(inputs, gate_matrix, preferred_element_type=jnp.float32)
        up_term = jnp.dot(inputs, up_matrix, preferred_element_type=jnp.float32)
        act = (jax.nn.silu(gate_term) * up_term).astype(jnp.bfloat16)
        return jnp.dot(act, down_matrix, preferred_element_type=jnp.float32).astype(jnp.bfloat16)
    results = lax.map(run_expert, (slot_table, w_gate, w_up, w_down))
    flat_results = results.reshape(EXPERTS * blocks * CAP, D)
    routed = flat_results[places].reshape(token_count, TOP, D).astype(jnp.float32)
    mixture = lax.optimization_barrier(jnp.sum(gate_values[:, :, None] * routed, axis=1))
    outputs = (token_rows + mixture).astype(jnp.bfloat16)
    out_rows = outputs.astype(jnp.float32)
    cosine = lax.optimization_barrier(jnp.mean(token_rows * out_rows, axis=1)) * lax.rsqrt((lax.optimization_barrier(jnp.mean(token_rows * token_rows, axis=1)) + EPS_COS) * (lax.optimization_barrier(jnp.mean(out_rows * out_rows, axis=1)) + EPS_COS))
    layer_score = jnp.mean(1.0 - cosine)
    return (outputs.reshape(SEQS, LEN, D), layer_score)
```

```python
import functools

import jax
import jax.numpy as jnp
from jax import lax
from jax.experimental import pallas as pl
from jax.experimental.pallas import tpu as pltpu
from jax.sharding import PartitionSpec as P

EPS_NORM = 1e-05
EPS_COS = 1e-06
BF = jnp.bfloat16
F32 = jnp.float32
RING = 4
MAIN = 16


class Links:
    def __init__(self, send_sems, recv_sems):
        self.send_sems, self.recv_sems, self.count, self.started = send_sems, recv_sems, 0, []

    def send(self, src, dst, device):
        n = self.count
        self.count += 1
        copy = pltpu.make_async_remote_copy(
            src_ref=src,
            dst_ref=dst,
            send_sem=self.send_sems.at[n],
            recv_sem=self.recv_sems.at[n],
            device_id=device,
            device_id_type=pl.DeviceIdType.MESH,
        )
        copy.start()
        self.started.append(copy)
        return copy

    def drain(self):
        for copy in self.started:
            copy.wait_send()


def mod(value, n):
    return lax.rem(value + 2 * n, n)


def dot(a, b):
    return jnp.dot(a, b, preferred_element_type=F32)


def onehot(mask):
    return jnp.where(mask, 1.0, 0.0).astype(BF)


def kernel(
    sizes,
    h_ref, ids_ref, gain_ref, router_ref, wg_hbm, wu_hbm, wd_hbm,
    out_ref, score_ref,
    wg, wu, wd, normed, keep, sent, got, back_sent, back,
    xa, xb, ga, ua, act, pa, pb, qa, qb, ra, rb, ta, tb, sa, sb, res,
    sums, totals, grand,
    send_sems, recv_sems, weight_sems,
):
    experts, cap = sizes
    tokens, width = h_ref.shape
    share = width // RING
    lanes = share // RING
    rows = experts * cap
    spread_rows = experts * MAIN
    per_lane = MAIN // 2
    z = lax.axis_index("expert")
    t = lax.axis_index("tensor")
    d = lax.axis_index("dp")
    x, c = d // 2, lax.rem(d, 2)
    other = 1 - c
    x_of = lambda pos: {"dp": pos * 2 + c}
    y_of = lambda pos: {"tensor": pos}
    partner = {"dp": x * 2 + other}
    dp_count = RING * 2

    barrier = pltpu.get_barrier_semaphore()
    peers = (
        [{"expert": mod(z + k, experts)} for k in range(1, experts)]
        + [{"tensor": mod(t + k, RING)} for k in range(1, RING)]
        + [{"dp": mod(d + k, dp_count)} for k in range(1, dp_count)]
    )
    for peer in peers:
        pl.semaphore_signal(barrier, inc=1, device_id=peer, device_id_type=pl.DeviceIdType.MESH)

    weights = [
        pltpu.make_async_copy(src, dst, weight_sems.at[n])
        for n, (src, dst) in enumerate(((wg_hbm, wg), (wu_hbm, wu), (wd_hbm, wd)))
    ]
    for copy in weights:
        copy.start()

    token_rows = h_ref[...].astype(F32)
    in_squares = jnp.sum(token_rows * token_rows, axis=1, keepdims=True) / width
    normed[...] = (token_rows * lax.rsqrt(in_squares + EPS_NORM) * gain_ref[...]).astype(BF)
    logits = dot(normed[...], router_ref[...])
    lane = lax.broadcasted_iota(jnp.int32, (tokens, 128), 1)
    lane_f = lane.astype(F32)
    first, second = ids_ref[:, 0:1], ids_ref[:, 1:2]
    first_f, second_f = first.astype(F32), second.astype(F32)
    is_first = jnp.where(lane == first, 1.0, 0.0)
    is_second = jnp.where(lane == second, 1.0, 0.0)
    spread = jnp.sum((is_first[:, :experts] - is_second[:, :experts]) * logits, axis=1, keepdims=True)
    gate_first = 1.0 / (1.0 + jnp.exp(-spread))
    gate_second = 1.0 / (1.0 + jnp.exp(spread))
    earlier = onehot(
        lax.broadcasted_iota(jnp.int32, (tokens, tokens), 1)
        < lax.broadcasted_iota(jnp.int32, (tokens, tokens), 0)
    )
    before = dot(earlier, (is_first + is_second).astype(BF))
    kept = [in_squares, gate_first, gate_second]
    for chosen, mask in ((first_f, is_first), (second_f, is_second)):
        slot = jnp.sum(before * mask, axis=1, keepdims=True)
        place = chosen * MAIN + slot
        kept.append(jnp.where(slot < MAIN, place, -1.0))
        kept.append(jnp.where(slot < MAIN, -1000.0, place - MAIN))
    for n, column in enumerate(kept):
        keep[n] = jnp.broadcast_to(column, (tokens, 128))

    def chosen_masks(n, shift):
        return onehot(lane_f - shift == keep[n])

    main = (chosen_masks(3, 0.0) + chosen_masks(5, 0.0)).astype(F32).T.astype(BF)
    extra = jnp.zeros((spread_rows, 128), F32)
    for k in range(per_lane):
        picks = (chosen_masks(4, 2.0 * k) + chosen_masks(6, 2.0 * k)).astype(F32).T.astype(BF)
        block = normed[:, pl.ds(pl.multiple_of(t * share + k * 128, 128), 128)]
        extra = extra + dot(picks[:spread_rows], block)
    for q in range(RING):
        block = normed[:, pl.ds(pl.multiple_of(t * share + q * lanes, 128), lanes)]
        picked = dot(main[:spread_rows], block).astype(BF)
        sent[:, :, q * lanes : (q + 1) * lanes] = picked.reshape(experts, MAIN, lanes)
    sent[:, :, share:] = extra.astype(BF).reshape(experts, MAIN, 128)

    ga[...] = jnp.zeros_like(ga)
    ua[...] = jnp.zeros_like(ua)
    pl.semaphore_wait(barrier, len(peers))
    links = Links(send_sems, recv_sems)

    def exchange(src, dst):
        copies = []
        for k in sorted(range(1, experts), key=lambda k: -min(k, experts - k)):
            to = mod(z + k, experts)
            copies.append(links.send(src.at[to], dst.at[z], {"expert": to}))
        dst[z] = src[z]
        for copy in copies:
            copy.wait_recv()

    exchange(sent, got)

    def placing(transposed):
        shape = (spread_rows, rows) if transposed else (rows, spread_rows)
        row = lax.broadcasted_iota(jnp.int32, shape, 1 if transposed else 0)
        place = lax.broadcasted_iota(jnp.int32, shape, 0 if transposed else 1)
        source, slot = place // MAIN, place % MAIN
        base = source * cap
        fits = (MAIN + slot % 2) < cap
        extras = [
            onehot((row == base + MAIN + slot % 2) & (slot // 2 == k) & fits) for k in range(per_lane)
        ]
        return onehot((row == base + slot) & (slot < cap)), extras

    put, put_extra = placing(False)
    extras = got[:, :, share:].reshape(spread_rows, 128)
    for q in range(RING):
        block = dot(put, got[:, :, q * lanes : (q + 1) * lanes].reshape(spread_rows, lanes))
        halves = [dot(put_extra[k], extras) for k in range(q * lanes // 128, (q + 1) * lanes // 128)]
        block = (block + jnp.concatenate(halves, axis=1)).astype(BF)
        if q < 2:
            xa[x, q, t, c] = block
        else:
            xb[t, q - 2, x, c] = block

    class Gather:
        def __init__(self, view, me, device_of):
            self.view = view
            self.left, self.right = mod(me - 1, RING), mod(me + 1, RING)
            self.to_left, self.to_right = device_of(self.left), device_of(self.right)
            send = lambda pos, q, to: links.send(view(pos, q), view(pos, q), to)
            self.from_left = [send(me, 0, self.to_right)]
            self.from_right = [send(me, 1, self.to_left)]
            self.from_left.append(send(me, 1, self.to_right))
            self.from_right.append(send(me, 0, self.to_left))

        def pass_on(self):
            self.from_left[0].wait_recv()
            left = self.view(self.left, 0)
            self.from_left.append(links.send(left, left, self.to_right))
            self.from_right[0].wait_recv()
            right = self.view(self.right, 1)
            self.from_right.append(links.send(right, right, self.to_left))

        def wait_left(self):
            self.from_left[1].wait_recv()

        def wait_right(self):
            self.from_right[1].wait_recv()

        def wait_far(self):
            self.from_left[2].wait_recv()
            self.from_right[2].wait_recv()

    small_a = Gather(lambda pos, q: xa.at[x, q, pos, c], t, y_of)
    small_b = Gather(lambda pos, q: xb.at[t, q, pos, c], x, x_of)
    small_a.pass_on()
    small_b.pass_on()
    for small in (small_a, small_b):
        small.wait_left()
        small.wait_right()
        small.wait_far()
    big_a = Gather(lambda pos, q: xa.at[pos, q, :, c], x, x_of)
    big_b = Gather(lambda pos, q: xb.at[pos, q, :, c], t, y_of)

    def share_core(buf, pos):
        return links.send(buf.at[pos, :, :, c], buf.at[pos, :, :, c], partner)

    m = 2 * rows

    def up_unit_a(pos):
        @pl.loop(0, RING)
        def _(y):
            for w, acc in ((wg, ga), (wu, ua)):
                terms = [dot(xa[pos, q, y].reshape(m, lanes), w[y * RING + q]) for q in range(2)]
                acc[pos] += terms[0] + terms[1]

    def up_unit_b(pos):
        @pl.loop(0, RING)
        def _(xp):
            for w, acc in ((wg, ga), (wu, ua)):
                terms = [dot(xb[pos, q, xp].reshape(m, lanes), w[pos * RING + 2 + q]) for q in range(2)]
                acc[xp] += terms[0] + terms[1]

    own_a, own_b = share_core(xa, x), share_core(xb, t)
    weights[0].wait()
    weights[1].wait()
    own_a.wait_recv()
    up_unit_a(x)
    own_b.wait_recv()
    up_unit_b(t)
    big_a.pass_on()
    big_b.pass_on()
    shared = []
    for big, buf, unit in ((big_a, xa, up_unit_a), (big_b, xb, up_unit_b)):
        big.wait_left()
        shared.append((share_core(buf, big.left), unit, big.left))
        big.wait_right()
        shared.append((share_core(buf, big.right), unit, big.right))
    for copy, unit, pos in shared:
        copy.wait_recv()
        unit(pos)
    far_x, far_y = mod(x + 2, RING), mod(t + 2, RING)
    big_a.wait_far()
    far_a = share_core(xa, far_x)
    big_b.wait_far()
    far_b = share_core(xb, far_y)
    far_a.wait_recv()
    up_unit_a(far_x)
    far_b.wait_recv()
    up_unit_b(far_y)

    weights[2].wait()

    @pl.loop(0, RING)
    def _(xp):
        gate = ga[xp]
        act[xp] = (gate / (1.0 + jnp.exp(-gate)) * ua[xp]).astype(BF)

    def down_unit_a(pos):
        @pl.loop(0, RING)
        def _(y):
            for q in range(2):
                w = wd[:, pl.ds(pl.multiple_of(y * share + q * lanes, 128), lanes)]
                pa[pos, q, y] = dot(act[pos], w).astype(BF).reshape(2, rows, lanes)

        return links.send(pa.at[pos, :, :, other], qa.at[pos], partner)

    def down_unit_b(pos):
        @pl.loop(0, RING)
        def _(xp):
            for q in range(2):
                w = wd[:, pl.ds(pl.multiple_of(pos * share + (2 + q) * lanes, 128), lanes)]
                pb[pos, q, xp] = dot(act[xp], w).astype(BF).reshape(2, rows, lanes)

        return links.send(pb.at[pos, :, :, other], qb.at[pos], partner)

    def add_pair(copy, part, came, pos):
        copy.wait_recv()

        @pl.loop(0, RING)
        def _(n):
            for q in range(2):
                part[pos, q, n, c] = (part[pos, q, n, c].astype(F32) + came[pos, q, n].astype(F32)).astype(BF)

    class Scatter:
        def __init__(self, view, slots, me, device_of):
            self.view, self.slots, self.me = view, slots, me
            self.left, self.right, self.far = mod(me - 1, RING), mod(me + 1, RING), mod(me + 2, RING)
            self.to_left, self.to_right = device_of(self.left), device_of(self.right)

        def send_far(self):
            self.rightward = [links.send(self.view(self.far, 0), self.slots.at[0], self.to_right)]
            self.leftward = [links.send(self.view(self.far, 1), self.slots.at[1], self.to_left)]

        def send_right(self):
            self.rightward.append(links.send(self.view(self.right, 1), self.slots.at[2], self.to_right))

        def send_left(self):
            self.leftward.append(links.send(self.view(self.left, 0), self.slots.at[3], self.to_left))

        def send_sums(self, add):
            self.rightward[0].wait_recv()
            add(self.right, 0, self.slots.at[0])
            self.rightward.append(links.send(self.view(self.right, 0), self.slots.at[4], self.to_right))
            self.leftward[0].wait_recv()
            add(self.left, 1, self.slots.at[1])
            self.leftward.append(links.send(self.view(self.left, 1), self.slots.at[5], self.to_left))

        def wait(self):
            for copy in self.rightward[1:] + self.leftward[1:]:
                copy.wait_recv()

        def parts(self, q):
            return (self.slots.at[4], self.slots.at[3]) if q == 0 else (self.slots.at[2], self.slots.at[5])

    rs_a = Scatter(lambda pos, q: pa.at[pos, q, :, c], ra, x, x_of)
    rs_b = Scatter(lambda pos, q: pb.at[pos, q, :, c], rb, t, y_of)

    def adder(part):
        def add(pos, q, slot):
            @pl.loop(0, RING)
            def _(n):
                part[pos, q, n, c] = (part[pos, q, n, c].astype(F32) + slot[n].astype(F32)).astype(BF)

        return add

    pair_a, pair_b = down_unit_a(far_x), down_unit_b(far_y)
    add_pair(pair_a, pa, qa, far_x)
    rs_a.send_far()
    pair_a = down_unit_a(rs_a.right)
    add_pair(pair_b, pb, qb, far_y)
    rs_b.send_far()
    pair_b = down_unit_b(rs_b.right)
    add_pair(pair_a, pa, qa, rs_a.right)
    rs_a.send_right()
    pair_a = down_unit_a(rs_a.left)
    add_pair(pair_b, pb, qb, rs_b.right)
    rs_b.send_right()
    pair_b = down_unit_b(rs_b.left)
    add_pair(pair_a, pa, qa, rs_a.left)
    rs_a.send_left()
    pair_a = down_unit_a(x)
    add_pair(pair_b, pb, qb, rs_b.left)
    rs_b.send_left()
    pair_b = down_unit_b(t)
    rs_a.send_sums(adder(pa))
    rs_b.send_sums(adder(pb))
    add_pair(pair_a, pa, qa, x)
    add_pair(pair_b, pb, qb, t)

    def finish_big(scatter, part, total, me):
        scatter.wait()

        @pl.loop(0, RING)
        def _(n):
            for q in range(2):
                one, two = scatter.parts(q)
                value = part[me, q, n, c].astype(F32) + one[n].astype(F32) + two[n].astype(F32)
                total[n, q] = value.astype(BF)

    finish_big(rs_a, pa, ta, x)
    last_a = Scatter(lambda pos, q: ta.at[pos, q], sa, t, y_of)
    last_a.send_far()
    last_a.send_right()
    last_a.send_left()
    finish_big(rs_b, pb, tb, t)
    last_b = Scatter(lambda pos, q: tb.at[pos, q], sb, x, x_of)
    last_b.send_far()
    last_b.send_right()
    last_b.send_left()

    def small_adder(total):
        def add(pos, q, slot):
            total[pos, q] = (total[pos, q].astype(F32) + slot[...].astype(F32)).astype(BF)

        return add

    last_a.send_sums(small_adder(ta))
    last_b.send_sums(small_adder(tb))
    for first_q, scatter, total in ((0, last_a, ta), (2, last_b, tb)):
        scatter.wait()
        for q in range(2):
            one, two = scatter.parts(q)
            value = total[scatter.me, q].astype(F32) + one[...].astype(F32) + two[...].astype(F32)
            res[first_q + q] = value.astype(BF)

    take, take_extra = placing(True)
    extra = jnp.zeros((spread_rows, 128), F32)
    for q in range(RING):
        block = res[q]
        back_sent[:, :, q * lanes : (q + 1) * lanes] = dot(take, block).astype(BF).reshape(experts, MAIN, lanes)
        for k in range(lanes // 128):
            extra = extra + dot(take_extra[q * lanes // 128 + k], block[:, k * 128 : (k + 1) * 128])
    back_sent[:, :, share:] = extra.astype(BF).reshape(experts, MAIN, 128)
    exchange(back_sent, back)

    extras = back[:, :, share:].reshape(spread_rows, 128)
    cross = jnp.zeros((tokens, 1), F32)
    squares = jnp.zeros((tokens, 1), F32)
    for k in range(share // 128):
        block = back[:, :, k * 128 : (k + 1) * 128].reshape(spread_rows, 128)
        mixture = jnp.zeros((tokens, 128), F32)
        for gate, n in ((1, 3), (2, 5)):
            picked = dot(chosen_masks(n, 0.0)[:, :spread_rows], block)
            picked = picked + dot(chosen_masks(n + 1, 2.0 * k)[:, :spread_rows], extras)
            mixture = mixture + keep[gate] * picked
        own = h_ref[:, pl.ds(pl.multiple_of(t * share + k * 128, 128), 128)].astype(F32)
        output = (own + mixture).astype(BF)
        out_ref[:, k * 128 : (k + 1) * 128] = output
        output = output.astype(F32)
        cross = cross + jnp.sum(own * output, axis=1, keepdims=True)
        squares = squares + jnp.sum(output * output, axis=1, keepdims=True)

    def total_over(buf, me, count, axis):
        copies = [
            links.send(buf.at[me], buf.at[me], {axis: mod(me + k, count)}) for k in range(1, count)
        ]
        for copy in copies:
            copy.wait_recv()
        total = buf[0]
        for n in range(1, count):
            total = total + buf[n]
        return total

    sums[t] = jnp.where(lane == 0, cross, jnp.where(lane == 1, squares, 0.0))
    both = total_over(sums, t, RING, "tensor")
    in_mean = keep[0][:, 0:1]
    cosine = both[:, 0:1] / width * lax.rsqrt((in_mean + EPS_COS) * (both[:, 1:2] / width + EPS_COS))
    local = jnp.sum(1.0 - cosine, axis=0, keepdims=True)
    totals[z] = jnp.broadcast_to(local, totals.shape[1:])
    grand[d] = total_over(totals, z, experts, "expert")
    score_ref[...] = total_over(grand, d, dp_count, "dp") / (tokens * experts * dp_count)
    links.drain()


def shards(hidden_in, expert_ids, ffn_gain, w_router, w_gate, w_up, w_down):
    tokens, width = hidden_in.shape[1:]
    top = expert_ids.shape[2]
    experts = lax.axis_size("expert")
    hidden = w_gate.shape[2]
    cap = max(2, 9 * tokens * top // (8 * experts))
    share = width // RING
    lanes = share // RING
    rows = experts * cap
    piece = (experts, MAIN, share + 128)
    vmem = pl.BlockSpec(memory_space=pltpu.VMEM)
    hbm = pl.BlockSpec(memory_space=pl.ANY)
    scratch = lambda shape, kind: pltpu.VMEM(shape, kind)
    copies = 160
    blocks = (RING, 2, RING, 2, rows, lanes)
    out, score = pl.pallas_call(
        functools.partial(kernel, (experts, cap)),
        out_shape=(
            jax.ShapeDtypeStruct((tokens, share), BF),
            jax.ShapeDtypeStruct((8, 128), F32),
        ),
        in_specs=[vmem] * 4 + [hbm] * 3,
        out_specs=(vmem, vmem),
        scratch_shapes=[
            scratch((width // lanes, lanes, hidden), BF),
            scratch((width // lanes, lanes, hidden), BF),
            scratch((hidden, width), BF),
            scratch((tokens, width), BF),
            scratch((8, tokens, 128), F32),
            scratch(piece, BF),
            scratch(piece, BF),
            scratch(piece, BF),
            scratch(piece, BF),
            scratch(blocks, BF),
            scratch(blocks, BF),
            scratch((RING, 2 * rows, hidden), F32),
            scratch((RING, 2 * rows, hidden), F32),
            scratch((RING, 2 * rows, hidden), BF),
            scratch(blocks, BF),
            scratch(blocks, BF),
            scratch((RING, 2, RING, rows, lanes), BF),
            scratch((RING, 2, RING, rows, lanes), BF),
            scratch((6, RING, rows, lanes), BF),
            scratch((6, RING, rows, lanes), BF),
            scratch((RING, 2, rows, lanes), BF),
            scratch((RING, 2, rows, lanes), BF),
            scratch((6, rows, lanes), BF),
            scratch((6, rows, lanes), BF),
            scratch((RING, rows, lanes), BF),
            scratch((RING, tokens, 128), F32),
            scratch((experts, 8, 128), F32),
            scratch((2 * RING, 8, 128), F32),
            pltpu.SemaphoreType.DMA((copies,)),
            pltpu.SemaphoreType.DMA((copies,)),
            pltpu.SemaphoreType.DMA((3,)),
        ],
        compiler_params=pltpu.CompilerParams(
            collective_id=0, has_side_effects=True, vmem_limit_bytes=67043328
        ),
        name="layer",
    )(
        hidden_in.reshape(tokens, width),
        expert_ids.reshape(tokens, top),
        ffn_gain.reshape(1, width),
        w_router,
        w_gate.reshape(width // lanes, lanes, hidden),
        w_up.reshape(width // lanes, lanes, hidden),
        w_down.reshape(hidden, width),
    )
    return out.reshape(1, tokens, share), score[0, 0]


def solution(mesh):
    return jax.shard_map(
        shards,
        mesh=mesh,
        in_specs=(
            P("dp", "expert", None),
            P("dp", "expert", None),
            P(),
            P(),
            P("expert", None, ("tensor", "dp")),
            P("expert", None, ("tensor", "dp")),
            P("expert", ("tensor", "dp"), None),
        ),
        out_specs=(P("dp", "expert", "tensor"), P()),
        check_vma=False,
    )
```

```python
import functools

import jax
import jax.numpy as jnp
from jax import lax
from jax.experimental import pallas as pl
from jax.experimental.pallas import tpu as pltpu
from jax.sharding import PartitionSpec as P

EPS_NORM = 1e-05
EPS_COS = 1e-06
BF = jnp.bfloat16
F32 = jnp.float32
RING = 4
SENDS = 64
MAIN = 16


class Links:
    def __init__(self, send_sems, recv_sems):
        self.send_sems, self.recv_sems, self.groups, self.started = send_sems, recv_sems, 0, []

    def group(self):
        self.groups += 1
        return self.groups - 1

    def send(self, src, dst, device, group=None):
        n = len(self.started)
        if n >= SENDS:
            self.started[n - SENDS].wait_send()
        copy = pltpu.make_async_remote_copy(
            src_ref=src,
            dst_ref=dst,
            send_sem=self.send_sems.at[n % SENDS],
            recv_sem=self.recv_sems.at[self.group() if group is None else group],
            device_id=device,
            device_id_type=pl.DeviceIdType.MESH,
        )
        copy.start()
        self.started.append(copy)
        return copy

    def arrived(self, group, whole, device):
        pltpu.make_async_remote_copy(
            src_ref=whole,
            dst_ref=whole,
            send_sem=self.send_sems.at[0],
            recv_sem=self.recv_sems.at[group],
            device_id=device,
            device_id_type=pl.DeviceIdType.MESH,
        ).wait_recv()

    def drain(self):
        for copy in self.started[-SENDS:]:
            copy.wait_send()


def mod(value, n):
    return lax.rem(value + 2 * n, n)


def dot(a, b):
    return jnp.dot(a, b, preferred_element_type=F32)


def dot_rows(a, b):
    return lax.dot_general(a, b, (((1,), (1,)), ((), ())), preferred_element_type=F32)


def onehot(mask):
    return jnp.where(mask, 1.0, 0.0).astype(BF)


def kernel(
    sizes,
    h_hbm, ids_hbm, gain_hbm, router_hbm, wg_hbm, wu_hbm, wd_hbm,
    out_hbm, score_ref,
    h_ref, ids_ref, gain_ref, router_ref, out_ref,
    wg, wu, wd, normed, keep, sent, got, back_sent, back,
    xa, xb, ga, ua, act, pa, pb, qa, qb, ra, rb, ta, tb, sa, sb, res,
    sums, totals, grand,
    send_sems, recv_sems, weight_sems,
):
    experts, cap = sizes
    tokens, width = h_hbm.shape
    share = width // RING
    lanes = share // RING
    rows = experts * cap
    spread_rows = experts * MAIN
    per_lane = MAIN // 2
    z = lax.axis_index("expert")
    t = lax.axis_index("tensor")
    d = lax.axis_index("dp")
    x, c = d // 2, lax.rem(d, 2)
    other = 1 - c
    x_of = lambda pos: {"dp": pos * 2 + c}
    y_of = lambda pos: {"tensor": pos}
    partner = {"dp": x * 2 + other}
    dp_count = RING * 2

    barrier = pltpu.get_barrier_semaphore()
    peers = (
        [{"expert": mod(z + k, experts)} for k in range(1, experts)]
        + [{"tensor": mod(t + k, RING)} for k in range(1, RING)]
        + [{"dp": mod(d + k, dp_count)} for k in range(1, dp_count)]
    )
    for peer in peers:
        pl.semaphore_signal(barrier, inc=1, device_id=peer, device_id_type=pl.DeviceIdType.MESH)

    weights = [
        pltpu.make_async_copy(src, dst, weight_sems.at[n])
        for n, (src, dst) in enumerate(
            (
                (wg_hbm, wg), (wu_hbm, wu), (wd_hbm, wd),
                (h_hbm, h_ref), (ids_hbm, ids_ref), (gain_hbm, gain_ref), (router_hbm, router_ref),
            )
        )
    ]
    for copy in weights[3:] + weights[:3]:
        copy.start()
    for copy in weights[3:]:
        copy.wait()

    token_rows = h_ref[...].astype(F32)
    in_squares = jnp.sum(token_rows * token_rows, axis=1, keepdims=True) / width
    normed[...] = (token_rows * lax.rsqrt(in_squares + EPS_NORM) * gain_ref[...]).astype(BF)
    logits = dot_rows(normed[...], router_ref[...])
    lane = lax.broadcasted_iota(jnp.int32, (tokens, 128), 1)
    lane_f = lane.astype(F32)
    ids = ids_ref[...].astype(F32)
    row_of = lax.broadcasted_iota(jnp.int32, (tokens, tokens), 0)
    lane_of = lax.broadcasted_iota(jnp.int32, (tokens, tokens), 1)
    first_f, second_f = (
        jnp.sum(jnp.where(row_of == lane_of, ids[n : n + 1], 0.0), axis=1, keepdims=True) for n in range(2)
    )
    is_first = jnp.where(lane_f == first_f, 1.0, 0.0)
    is_second = jnp.where(lane_f == second_f, 1.0, 0.0)
    spread = jnp.sum((is_first[:, :experts] - is_second[:, :experts]) * logits, axis=1, keepdims=True)
    gate_first = 1.0 / (1.0 + jnp.exp(-spread))
    gate_second = 1.0 / (1.0 + jnp.exp(spread))
    before = dot(onehot(lane_of < row_of), (is_first + is_second).astype(BF))
    kept = [in_squares, gate_first, gate_second]
    for chosen, mask in ((first_f, is_first), (second_f, is_second)):
        slot = jnp.sum(before * mask, axis=1, keepdims=True)
        place = chosen * MAIN + slot
        kept.append(jnp.where(slot < MAIN, place, -1.0))
        kept.append(jnp.where(slot < MAIN, -1000.0, place - MAIN))
    for n, column in enumerate(kept):
        keep[n] = jnp.broadcast_to(column, (tokens, 128))

    def chosen_masks(n, shift):
        return onehot(lane_f - shift == keep[n])

    main = (chosen_masks(3, 0.0) + chosen_masks(5, 0.0)).astype(F32).T.astype(BF)
    extra = jnp.zeros((spread_rows, 128), F32)
    for k in range(per_lane):
        picks = (chosen_masks(4, 2.0 * k) + chosen_masks(6, 2.0 * k)).astype(F32).T.astype(BF)
        block = normed[:, pl.ds(pl.multiple_of(t * share + k * 128, 128), 128)]
        extra = extra + dot(picks[:spread_rows], block)
    def spot(q):
        return (q // 2) * lanes + (q % 2) * (2 * lanes + 128)

    extra_at = 2 * lanes
    for q in range(RING):
        block = normed[:, pl.ds(pl.multiple_of(t * share + q * lanes, 128), lanes)]
        picked = dot(main[:spread_rows], block).astype(BF)
        sent[:, :, spot(q) : spot(q) + lanes] = picked.reshape(experts, MAIN, lanes)
    sent[:, :, extra_at : extra_at + 128] = extra.astype(BF).reshape(experts, MAIN, 128)

    ga[...] = jnp.zeros_like(ga)
    ua[...] = jnp.zeros_like(ua)
    pl.semaphore_wait(barrier, len(peers))
    links = Links(send_sems, recv_sems)

    def exchange(src, dst, begin, end):
        group = links.group()
        for k in sorted(range(1, experts), key=lambda k: -min(k, experts - k)):
            to = mod(z + k, experts)
            links.send(src.at[to, :, begin:end], dst.at[z, :, begin:end], {"expert": to}, group)
        dst[z, :, begin:end] = src[z, :, begin:end]
        return group, dst.at[: experts - 1, :, begin:end]

    def received(exchanged):
        links.arrived(*exchanged, partner)

    arriving = [exchange(sent, got, 0, extra_at + 128), exchange(sent, got, extra_at + 128, share + 128)]

    def placing(transposed):
        shape = (spread_rows, rows) if transposed else (rows, spread_rows)
        row = lax.broadcasted_iota(jnp.int32, shape, 1 if transposed else 0)
        place = lax.broadcasted_iota(jnp.int32, shape, 0 if transposed else 1)
        source, slot = place // MAIN, place % MAIN
        base = source * cap
        fits = (MAIN + slot % 2) < cap
        extras = [
            onehot((row == base + MAIN + slot % 2) & (slot // 2 == k) & fits) for k in range(per_lane)
        ]
        return onehot((row == base + slot) & (slot < cap)), extras

    put, put_extra = placing(False)

    def compact(j):
        extras = got[:, :, extra_at : extra_at + 128].reshape(spread_rows, 128)
        for q in (j, 2 + j):
            block = dot(put, got[:, :, spot(q) : spot(q) + lanes].reshape(spread_rows, lanes))
            halves = [dot(put_extra[k], extras) for k in range(q * lanes // 128, (q + 1) * lanes // 128)]
            block = (block + jnp.concatenate(halves, axis=1)).astype(BF)
            if q < 2:
                xa[x, j, t, c] = block
            else:
                xb[t, j, x, c] = block

    half = lanes // 2

    def part_of(h):
        return pl.ds(h * half, half)

    class Gather:
        def __init__(self, view, block, me, device_of):
            self.view, self.block = view, block
            self.left, self.right, self.far = mod(me - 1, RING), mod(me + 1, RING), mod(me + 2, RING)
            self.to_left, self.to_right = device_of(self.left), device_of(self.right)
            send = lambda pos, h, to: links.send(view(pos, h), view(pos, h), to)
            self.from_left = [send(me, 0, self.to_right)]
            self.from_right = [send(me, 1, self.to_left)]
            self.from_left.append(send(me, 1, self.to_right))
            self.from_right.append(send(me, 0, self.to_left))

        def pass_on(self):
            self.from_left[0].wait_recv()
            self.pass_halves(self.from_right[0].wait_recv)

        def pass_halves(self, wait_other):
            self.far_group = links.group()
            left = self.view(self.left, 0)
            links.send(left, left, self.to_right, self.far_group)
            wait_other()
            right = self.view(self.right, 1)
            links.send(right, right, self.to_left, self.far_group)

        def wait_left(self):
            self.from_left[1].wait_recv()

        def wait_right(self):
            self.from_right[1].wait_recv()

        def wait_far(self):
            links.arrived(self.far_group, self.block(self.far), self.to_left)

    class PiecewiseGather(Gather):
        def __init__(self, view, block, piece, me, device_of, short):
            self.view, self.block, self.piece, self.me = view, block, piece, me
            self.left, self.right, self.far = mod(me - 1, RING), mod(me + 1, RING), mod(me + 2, RING)
            self.to_left, self.to_right = device_of(self.left), device_of(self.right)
            self.order = (mod(short, RING), mod(short - 1, RING), mod(short + 1, RING), mod(short + 2, RING))
            self.right_going = links.group(), links.group()
            self.left_going = links.group(), links.group()

        def feed(self, n):
            for turn in range(2):
                for h, going, to in (
                    (turn, self.right_going, self.to_right),
                    (1 - turn, self.left_going, self.to_left),
                ):
                    block = self.piece(self.me, h, self.order[n])
                    links.send(block, block, to, going[h])

        def arrived(self, going, pos, h):
            links.arrived(going[h], self.view(pos, h), self.to_left)

        def pass_on(self):
            self.arrived(self.right_going, self.left, 0)
            self.pass_halves(lambda: self.arrived(self.left_going, self.right, 1))

        def wait_left(self):
            self.arrived(self.right_going, self.left, 1)

        def wait_right(self):
            self.arrived(self.left_going, self.right, 0)

    def small_gathers(j):
        return (
            Gather(lambda pos, h: xa.at[x, j, pos, c, :, part_of(h)], lambda pos: xa.at[x, j, pos, c], t, y_of),
            Gather(lambda pos, h: xb.at[t, j, pos, c, :, part_of(h)], lambda pos: xb.at[t, j, pos, c], x, x_of),
        )

    def big_gathers(j):
        return (
            PiecewiseGather(
                lambda pos, h: xa.at[pos, j, :, c, :, part_of(h)],
                lambda pos: xa.at[pos, j, :, c],
                lambda pos, h, n: xa.at[pos, j, n, c, :, part_of(h)],
                x, x_of, t,
            ),
            PiecewiseGather(
                lambda pos, h: xb.at[pos, j, :, c, :, part_of(h)],
                lambda pos: xb.at[pos, j, :, c],
                lambda pos, h, n: xb.at[pos, j, n, c, :, part_of(h)],
                t, y_of, x,
            ),
        )

    def feed_own(longs):
        for long in longs:
            long.feed(0)

    def feed_sides(shorts, longs):
        for short, long in zip(shorts, longs):
            short.wait_left()
            long.feed(1)
            short.wait_right()
            long.feed(2)

    def feed_far(shorts, longs):
        for short, long in zip(shorts, longs):
            short.wait_far()
            long.feed(3)

    def pass_on(gathers):
        for gather in gathers:
            gather.pass_on()

    def share_core(buf, pos, j):
        return links.send(buf.at[pos, j, :, c], buf.at[pos, j, :, c], partner)

    m = 2 * rows

    def columns(w, n):
        return w[:, pl.ds(pl.multiple_of(n * lanes, 128), lanes)]

    def up_a(copy, pos, j):
        copy.wait_recv()

        tokens_in = jnp.concatenate([xa[pos, j, y].reshape(m, lanes) for y in range(RING)], axis=1)
        for w, acc in ((wg, ga), (wu, ua)):
            columns_in = jnp.concatenate([columns(w, y * RING + j) for y in range(RING)], axis=1)
            acc[pos] += dot_rows(tokens_in, columns_in)

    def up_b(copy, pos, j):
        copy.wait_recv()

        for w, acc in ((wg, ga), (wu, ua)):
            product = dot_rows(xb[pos, j].reshape(RING * m, lanes), columns(w, pos * RING + 2 + j))
            acc[...] += product.reshape(acc.shape)

    def share_sides(gathers, j):
        shared = []
        for gather, buf, unit in zip(gathers, (xa, xb), (up_a, up_b)):
            gather.wait_left()
            shared.append((unit, share_core(buf, gather.left, j), gather.left))
            gather.wait_right()
            shared.append((unit, share_core(buf, gather.right, j), gather.right))
        return shared

    def share_far(gathers, j):
        shared = []
        for gather, buf, unit in zip(gathers, (xa, xb), (up_a, up_b)):
            gather.wait_far()
            shared.append((unit, share_core(buf, gather.far, j), gather.far))
        return shared

    def run(shared, j):
        for unit, copy, pos in shared:
            unit(copy, pos, j)

    received(arriving[0])
    compact(0)
    small_0, big_0 = small_gathers(0), big_gathers(0)
    feed_own(big_0)
    pass_on(small_0)
    received(arriving[1])
    compact(1)
    small_1, big_1 = small_gathers(1), big_gathers(1)
    feed_sides(small_0, big_0)
    feed_far(small_0, big_0)
    own_0 = [(up_a, share_core(xa, x, 0), x), (up_b, share_core(xb, t, 0), t)]
    feed_own(big_1)
    pass_on(small_1)
    weights[0].wait()
    weights[1].wait()
    run(own_0, 0)
    feed_sides(small_1, big_1)
    feed_far(small_1, big_1)
    own_1 = [(up_a, share_core(xa, x, 1), x), (up_b, share_core(xb, t, 1), t)]
    pass_on(big_0)
    run(own_1, 1)
    sides_0 = share_sides(big_0, 0)
    run(sides_0, 0)
    pass_on(big_1)
    sides_1 = share_sides(big_1, 1)
    run(sides_1[:2], 1)
    far_0 = share_far(big_0, 0)
    run(sides_1[2:], 1)
    run(far_0[:1], 0)
    far_1 = share_far(big_1, 1)
    run(far_0[1:], 0)
    run(far_1, 1)

    weights[2].wait()

    @pl.loop(0, RING)
    def _(xp):
        gate = ga[xp]
        act[xp] = (gate / (1.0 + jnp.exp(-gate)) * ua[xp]).astype(BF)

    def down_a(pos, j):
        columns_in = jnp.concatenate([columns(wd, y * RING + j) for y in range(RING)], axis=1)
        product = dot(act[pos], columns_in).astype(BF)
        for y in range(RING):
            pa[pos, j, y] = product[:, y * lanes : (y + 1) * lanes].reshape(2, rows, lanes)

        return links.send(pa.at[pos, j, :, other], qa.at[pos, j], partner)

    def down_b(pos, j):
        product = dot(act[...].reshape(RING * m, act.shape[2]), columns(wd, pos * RING + 2 + j)).astype(BF)
        pb[pos, j] = product.reshape(RING, 2, rows, lanes)

        return links.send(pb.at[pos, j, :, other], qb.at[pos, j], partner)

    def add_pair(copy, part, came, pos, j):
        copy.wait_recv()

        @pl.loop(0, RING)
        def _(n):
            part[pos, j, n, c] = (part[pos, j, n, c].astype(F32) + came[pos, j, n].astype(F32)).astype(BF)

    class Scatter:
        def __init__(self, view, slots, me, device_of):
            self.view, self.slots, self.me = view, slots, me
            self.left, self.right, self.far = mod(me - 1, RING), mod(me + 1, RING), mod(me + 2, RING)
            self.to_left, self.to_right = device_of(self.left), device_of(self.right)

        def send_far(self):
            self.rightward = links.send(self.view(self.far, 0), self.slots.at[0], self.to_right)
            self.leftward = links.send(self.view(self.far, 1), self.slots.at[1], self.to_left)

            self.last_group = links.group()

        def send_right(self):
            links.send(self.view(self.right, 1), self.slots.at[2], self.to_right, self.last_group)

        def send_left(self):
            links.send(self.view(self.left, 0), self.slots.at[3], self.to_left, self.last_group)

        def send_sums(self, add):
            self.rightward.wait_recv()
            add(self.right, 0, self.slots.at[0])
            links.send(self.view(self.right, 0), self.slots.at[4], self.to_right, self.last_group)
            self.leftward.wait_recv()
            add(self.left, 1, self.slots.at[1])
            links.send(self.view(self.left, 1), self.slots.at[5], self.to_left, self.last_group)

        def wait(self):
            links.arrived(self.last_group, self.slots.at[2:6], self.to_left)

        def parts(self, h):
            return (self.slots.at[4], self.slots.at[3]) if h == 0 else (self.slots.at[2], self.slots.at[5])

    def big_a(j):
        return Scatter(lambda pos, h: pa.at[pos, j, :, c, :, part_of(h)], ra.at[j], x, x_of)

    def big_b(j):
        return Scatter(lambda pos, h: pb.at[pos, j, :, c, :, part_of(h)], rb.at[j], t, y_of)

    def adder(part, j):
        def add(pos, h, slot):
            @pl.loop(0, RING)
            def _(n):
                own = part[pos, j, n, c, :, part_of(h)].astype(F32)
                part[pos, j, n, c, :, part_of(h)] = (own + slot[n].astype(F32)).astype(BF)

        return add

    rs_a, rs_b = [big_a(0), big_a(1)], [big_b(0), big_b(1)]
    pair_a, pair_b = down_a(rs_a[0].far, 0), down_b(rs_b[0].far, 0)
    for j in range(2):
        one, two = rs_a[j], rs_b[j]
        add_pair(pair_a, pa, qa, one.far, j)
        one.send_far()
        pair_a = down_a(one.right, j)
        add_pair(pair_b, pb, qb, two.far, j)
        two.send_far()
        pair_b = down_b(two.right, j)
        add_pair(pair_a, pa, qa, one.right, j)
        one.send_right()
        pair_a = down_a(one.left, j)
        add_pair(pair_b, pb, qb, two.right, j)
        two.send_right()
        pair_b = down_b(two.left, j)
        add_pair(pair_a, pa, qa, one.left, j)
        one.send_left()
        pair_a = down_a(one.far, 1) if j == 0 else down_a(x, 0)
        add_pair(pair_b, pb, qb, two.left, j)
        two.send_left()
        pair_b = down_b(two.far, 1) if j == 0 else down_b(t, 0)
        if j == 0:
            one.send_sums(adder(pa, j))
            two.send_sums(adder(pb, j))
    own_a, own_b = down_a(x, 1), down_b(t, 1)
    add_pair(pair_a, pa, qa, x, 0)
    add_pair(pair_b, pb, qb, t, 0)

    def finish_big(scatter, part, total, me, j):
        scatter.wait()

        @pl.loop(0, RING)
        def _(n):
            for h in range(2):
                one, two = scatter.parts(h)
                value = part[me, j, n, c, :, part_of(h)].astype(F32)
                total[n, j, :, part_of(h)] = (value + one[n].astype(F32) + two[n].astype(F32)).astype(BF)

    def small_a(j):
        finish_big(rs_a[j], pa, ta, x, j)
        small = Scatter(lambda pos, h: ta.at[pos, j, :, part_of(h)], sa.at[j], t, y_of)
        small.send_far()
        small.send_right()
        small.send_left()
        return small

    def small_b(j):
        finish_big(rs_b[j], pb, tb, t, j)
        small = Scatter(lambda pos, h: tb.at[pos, j, :, part_of(h)], sb.at[j], x, x_of)
        small.send_far()
        small.send_right()
        small.send_left()
        return small

    def small_adder(total, j):
        def add(pos, h, slot):
            own = total[pos, j, :, part_of(h)].astype(F32)
            total[pos, j, :, part_of(h)] = (own + slot[...].astype(F32)).astype(BF)

        return add

    def finish_small(small, total, q, j):
        small.wait()
        for h in range(2):
            one, two = small.parts(h)
            value = total[small.me, j, :, part_of(h)].astype(F32)
            res[q, :, part_of(h)] = (value + one[...].astype(F32) + two[...].astype(F32)).astype(BF)

    take, take_extra = placing(True)

    def take_out(q):
        picked = dot(take, res[q]).astype(BF)
        back_sent[:, :, spot(q) : spot(q) + lanes] = picked.reshape(experts, MAIN, lanes)

    last_a, last_b = [small_a(0)], [small_b(0)]
    add_pair(own_a, pa, qa, x, 1)
    add_pair(own_b, pb, qb, t, 1)
    rs_a[1].send_sums(adder(pa, 1))
    rs_b[1].send_sums(adder(pb, 1))
    last_a[0].send_sums(small_adder(ta, 0))
    last_b[0].send_sums(small_adder(tb, 0))
    last_a.append(small_a(1))
    last_b.append(small_b(1))
    finish_small(last_a[0], ta, 0, 0)
    finish_small(last_b[0], tb, 2, 0)
    take_out(0)
    take_out(2)
    returning = [exchange(back_sent, back, 0, extra_at)]
    last_a[1].send_sums(small_adder(ta, 1))
    last_b[1].send_sums(small_adder(tb, 1))
    finish_small(last_a[1], ta, 1, 1)
    finish_small(last_b[1], tb, 3, 1)
    take_out(1)
    take_out(3)
    extra = jnp.zeros((spread_rows, 128), F32)
    for k in range(per_lane):
        q, at = k * 128 // lanes, k * 128 % lanes
        extra = extra + dot(take_extra[k], res[q, :, at : at + 128])
    back_sent[:, :, extra_at : extra_at + 128] = extra.astype(BF).reshape(experts, MAIN, 128)
    returning.append(exchange(back_sent, back, extra_at, share + 128))
    received(returning[0])
    received(returning[1])

    extras = back[:, :, extra_at : extra_at + 128].reshape(spread_rows, 128)
    cross = jnp.zeros((tokens, 1), F32)
    squares = jnp.zeros((tokens, 1), F32)
    for k in range(share // 128):
        at = spot(k * 128 // lanes) + k * 128 % lanes
        block = back[:, :, at : at + 128].reshape(spread_rows, 128)
        mixture = jnp.zeros((tokens, 128), F32)
        for gate, n in ((1, 3), (2, 5)):
            picked = dot(chosen_masks(n, 0.0)[:, :spread_rows], block)
            picked = picked + dot(chosen_masks(n + 1, 2.0 * k)[:, :spread_rows], extras)
            mixture = mixture + keep[gate] * picked
        own = h_ref[:, pl.ds(pl.multiple_of(t * share + k * 128, 128), 128)].astype(F32)
        output = (own + mixture).astype(BF)
        out_ref[:, k * 128 : (k + 1) * 128] = output
        output = output.astype(F32)
        cross = cross + jnp.sum(own * output, axis=1, keepdims=True)
        squares = squares + jnp.sum(output * output, axis=1, keepdims=True)

    out_copy = pltpu.make_async_copy(out_ref, out_hbm, weight_sems.at[7])
    out_copy.start()

    def total_over(buf, me, count, axis):
        group = links.group()
        for k in range(1, count):
            links.send(buf.at[me], buf.at[me], {axis: mod(me + k, count)}, group)
        links.arrived(group, buf.at[: count - 1], partner)
        total = buf[0]
        for n in range(1, count):
            total = total + buf[n]
        return total

    sums[t] = jnp.where(lane == 0, cross, jnp.where(lane == 1, squares, 0.0))
    both = total_over(sums, t, RING, "tensor")
    in_mean = keep[0][:, 0:1]
    cosine = both[:, 0:1] / width * lax.rsqrt((in_mean + EPS_COS) * (both[:, 1:2] / width + EPS_COS))
    local = jnp.sum(1.0 - cosine, axis=0, keepdims=True)
    totals[z] = jnp.broadcast_to(local, totals.shape[1:])
    grand[d] = total_over(totals, z, experts, "expert")
    score = total_over(grand, d, dp_count, "dp") / (tokens * experts * dp_count)
    score_ref[0, 0] = score[0, 0]
    out_copy.wait()
    links.drain()


def shards(hidden_in, expert_ids, ffn_gain, w_router, w_gate, w_up, w_down):
    tokens, width = hidden_in.shape[1:]
    top = expert_ids.shape[2]
    experts = lax.axis_size("expert")
    hidden = w_gate.shape[2]
    cap = max(2, 9 * tokens * top // (8 * experts))
    share = width // RING
    lanes = share // RING
    rows = experts * cap
    piece = (experts, MAIN, share + 128)
    hbm = pl.BlockSpec(memory_space=pl.ANY)
    scratch = lambda shape, kind: pltpu.VMEM(shape, kind)
    blocks = (RING, 2, RING, 2, rows, lanes)
    out, score = pl.pallas_call(
        functools.partial(kernel, (experts, cap)),
        out_shape=(
            jax.ShapeDtypeStruct((tokens, share), BF),
            jax.ShapeDtypeStruct((1, 1), F32),
        ),
        in_specs=[hbm] * 7,
        out_specs=(hbm, pl.BlockSpec(memory_space=pltpu.SMEM)),
        scratch_shapes=[
            scratch((tokens, width), BF),
            scratch((top, tokens), jnp.int32),
            scratch((1, width), F32),
            scratch((experts, width), BF),
            scratch((tokens, share), BF),
            scratch((hidden, width), BF),
            scratch((hidden, width), BF),
            scratch((hidden, width), BF),
            scratch((tokens, width), BF),
            scratch((8, tokens, 128), F32),
            scratch(piece, BF),
            scratch(piece, BF),
            scratch(piece, BF),
            scratch(piece, BF),
            scratch(blocks, BF),
            scratch(blocks, BF),
            scratch((RING, 2 * rows, hidden), F32),
            scratch((RING, 2 * rows, hidden), F32),
            scratch((RING, 2 * rows, hidden), BF),
            scratch(blocks, BF),
            scratch(blocks, BF),
            scratch((RING, 2, RING, rows, lanes), BF),
            scratch((RING, 2, RING, rows, lanes), BF),
            scratch((2, 6, RING, rows, lanes // 2), BF),
            scratch((2, 6, RING, rows, lanes // 2), BF),
            scratch((RING, 2, rows, lanes), BF),
            scratch((RING, 2, rows, lanes), BF),
            scratch((2, 6, rows, lanes // 2), BF),
            scratch((2, 6, rows, lanes // 2), BF),
            scratch((RING, rows, lanes), BF),
            scratch((RING, tokens, 128), F32),
            scratch((experts, 8, 128), F32),
            scratch((2 * RING, 8, 128), F32),
            pltpu.SemaphoreType.DMA((SENDS,)),
            pltpu.SemaphoreType.DMA((103,)),
            pltpu.SemaphoreType.DMA((8,)),
        ],
        compiler_params=pltpu.CompilerParams(
            collective_id=0, has_side_effects=True, vmem_limit_bytes=67043328
        ),
        name="layer",
    )(
        hidden_in.reshape(tokens, width),
        expert_ids.reshape(tokens, top).T,
        ffn_gain.reshape(1, width),
        w_router.T,
        w_gate.reshape(width, hidden).T,
        w_up.reshape(width, hidden).T,
        w_down.reshape(hidden, width),
    )
    return out.reshape(1, tokens, share), score[0, 0]


def solution(mesh):
    return jax.shard_map(
        shards,
        mesh=mesh,
        in_specs=(
            P("dp", "expert", None),
            P("dp", "expert", None),
            P(),
            P(),
            P("expert", None, ("tensor", "dp")),
            P("expert", None, ("tensor", "dp")),
            P("expert", ("tensor", "dp"), None),
        ),
        out_specs=(P("dp", "expert", "tensor"), P()),
        check_vma=False,
    )
```

```python
import functools

import jax
import jax.numpy as jnp
from jax import lax
from jax.experimental import pallas as pl
from jax.experimental.pallas import tpu as pltpu
from jax.sharding import PartitionSpec as P

EPS_NORM = 1e-05
EPS_COS = 1e-06
BF = jnp.bfloat16
F32 = jnp.float32
RING = 4
SENDS = 64
MAIN = 16
SLOTS = (10, 8)
WIDE = 8


class Links:
    def __init__(self, send_sems, recv_sems):
        self.send_sems, self.recv_sems, self.groups, self.started = send_sems, recv_sems, 0, []

    def group(self):
        self.groups += 1
        return self.groups - 1

    def send(self, src, dst, device, group=None):
        n = len(self.started)
        if n >= SENDS:
            self.started[n - SENDS].wait_send()
        copy = pltpu.make_async_remote_copy(
            src_ref=src,
            dst_ref=dst,
            send_sem=self.send_sems.at[n % SENDS],
            recv_sem=self.recv_sems.at[self.group() if group is None else group],
            device_id=device,
            device_id_type=pl.DeviceIdType.MESH,
        )
        copy.start()
        self.started.append(copy)
        return copy

    def arrived(self, group, whole, device):
        pltpu.make_async_remote_copy(
            src_ref=whole,
            dst_ref=whole,
            send_sem=self.send_sems.at[0],
            recv_sem=self.recv_sems.at[group],
            device_id=device,
            device_id_type=pl.DeviceIdType.MESH,
        ).wait_recv()

    def drain(self):
        for copy in self.started[-SENDS:]:
            copy.wait_send()


def mod(value, n):
    return lax.rem(value + 2 * n, n)


def dot(a, b):
    return jnp.dot(a, b, preferred_element_type=F32)


def dot_rows(a, b):
    return lax.dot_general(a, b, (((1,), (1,)), ((), ())), preferred_element_type=F32)


def onehot(mask):
    return jnp.where(mask, 1.0, 0.0).astype(BF)


def kernel(
    sizes,
    h_hbm, ids_hbm, gain_hbm, router_hbm, wg_hbm, wu_hbm, wd_hbm,
    out_hbm, score_ref,
    h_ref, ids_ref, gain_ref, router_ref, out_ref,
    wg, wu, wd, turned_g, turned_u, normed, keep, sent, got, back_sent, back,
    *buffers,
):
    *buffers, mixed, sums, totals, grand, send_sems, recv_sems, weight_sems = buffers
    xa, xb, ga, ua, act, pa, pb, qa, qb, ra, rb, ta, tb, sa, sb, ea, eb = zip(buffers[::2], buffers[1::2])
    experts, cap = sizes
    tokens, width = h_hbm.shape
    share = width // RING
    lanes = share // 2
    rows = [experts * n for n in SLOTS]
    spread_rows = experts * MAIN
    blocks = share // 128
    z = lax.axis_index("expert")
    t = lax.axis_index("tensor")
    d = lax.axis_index("dp")
    x, c = d // 2, lax.rem(d, 2)
    other = 1 - c
    x_of = lambda pos: {"dp": pos * 2 + c}
    y_of = lambda pos: {"tensor": pos}
    partner = {"dp": x * 2 + other}
    dp_count = RING * 2

    barrier = pltpu.get_barrier_semaphore()
    peers = (
        [{"expert": mod(z + k, experts)} for k in range(1, experts)]
        + [{"tensor": mod(t + k, RING)} for k in range(1, RING)]
        + [{"dp": mod(d + k, dp_count)} for k in range(1, dp_count)]
    )
    for peer in peers:
        pl.semaphore_signal(barrier, inc=1, device_id=peer, device_id_type=pl.DeviceIdType.MESH)

    weights = [
        pltpu.make_async_copy(src, dst, weight_sems.at[n])
        for n, (src, dst) in enumerate(
            (
                (wg_hbm, wg), (wu_hbm, wu), (wd_hbm, wd),
                (h_hbm, h_ref), (ids_hbm, ids_ref), (gain_hbm, gain_ref), (router_hbm, router_ref),
            )
        )
    ]
    for copy in weights[3:] + weights[:3]:
        copy.start()
    for copy in weights[3:]:
        copy.wait()

    token_rows = h_ref[...].astype(F32)
    in_squares = jnp.sum(token_rows * token_rows, axis=1, keepdims=True) / width
    normed[...] = (token_rows * lax.rsqrt(in_squares + EPS_NORM) * gain_ref[...]).astype(BF)
    logits = dot_rows(normed[...], router_ref[...])
    lane = lax.broadcasted_iota(jnp.int32, (tokens, 128), 1)
    lane_f = lane.astype(F32)
    ids = ids_ref[...].astype(F32)
    row_of = lax.broadcasted_iota(jnp.int32, (tokens, tokens), 0)
    lane_of = lax.broadcasted_iota(jnp.int32, (tokens, tokens), 1)
    first_f, second_f = (
        jnp.sum(jnp.where(row_of == lane_of, ids[n : n + 1], 0.0), axis=1, keepdims=True) for n in range(2)
    )
    is_first = jnp.where(lane_f == first_f, 1.0, 0.0)
    is_second = jnp.where(lane_f == second_f, 1.0, 0.0)
    spread = jnp.sum((is_first[:, :experts] - is_second[:, :experts]) * logits, axis=1, keepdims=True)
    gate_first = 1.0 / (1.0 + jnp.exp(-spread))
    gate_second = 1.0 / (1.0 + jnp.exp(spread))
    before = dot(onehot(lane_of < row_of), (is_first + is_second).astype(BF))
    kept = [in_squares, gate_first, gate_second]
    for chosen, mask in ((first_f, is_first), (second_f, is_second)):
        slot = jnp.sum(before * mask, axis=1, keepdims=True)
        place = chosen * MAIN
        late = slot - SLOTS[0]
        kept.append(jnp.where(slot < WIDE, place + 2.0 * slot, -1000.0))
        kept.append(jnp.where((slot >= WIDE) & (late < 0.0), place + slot - WIDE, -1000.0))
        kept.append(jnp.where(late >= 0.0, place + 2.0 * late, -1000.0))
    for n, column in enumerate(kept):
        keep[n] = jnp.broadcast_to(column, (tokens, 128))

    def chosen_masks(n, shift):
        return onehot(lane_f - shift == keep[n])

    extra_at = lanes
    starts, ends = (0, lanes + 128), (lanes + 128, 2 * lanes + 128)

    def picks(n, shift):
        return (chosen_masks(n, shift) + chosen_masks(n + 3, shift)).astype(F32).T.astype(BF)[:spread_rows]

    def own_lanes(k):
        return pl.ds(pl.multiple_of(t * share + k * 128, 128), 128)

    for j in range(2):
        select = [picks(3 + 2 * j, float(b)) for b in range(2)]
        for p in range(blocks // 2):
            picked = sum(dot(select[b], normed[:, own_lanes(2 * p + b)]) for b in range(2))
            at = starts[j] + p * 128
            sent[:, :, at : at + 128] = picked.astype(BF).reshape(experts, MAIN, 128)
    extra = sum(dot(picks(4, 2.0 * k), normed[:, own_lanes(k)]) for k in range(blocks))
    sent[:, :, extra_at : extra_at + 128] = extra.astype(BF).reshape(experts, MAIN, 128)

    for acc in ga + ua:
        acc[...] = jnp.zeros_like(acc)
    pl.semaphore_wait(barrier, len(peers))
    links = Links(send_sems, recv_sems)

    def exchange(src, dst, begin, end):
        group = links.group()
        for k in sorted(range(1, experts), key=lambda k: -min(k, experts - k)):
            to = mod(z + k, experts)
            links.send(src.at[to, :, begin:end], dst.at[z, :, begin:end], {"expert": to}, group)
        dst[z, :, begin:end] = src[z, :, begin:end]
        return group, dst.at[: experts - 1, :, begin:end]

    def received(exchanged):
        links.arrived(*exchanged, partner)

    arriving = [exchange(sent, got, starts[j], ends[j]) for j in range(2)]

    def placing(j, transposed):
        shape = (spread_rows, rows[j]) if transposed else (rows[j], spread_rows)
        row = lax.broadcasted_iota(jnp.int32, shape, 1 if transposed else 0)
        place = lax.broadcasted_iota(jnp.int32, shape, 0 if transposed else 1)
        base, within = place // MAIN * SLOTS[j], place % MAIN
        wide = [onehot((row == base + within // 2) & (within % 2 == b)) for b in range(2)]
        extras = [onehot((row == base + WIDE + within % 2) & (within // 2 == k)) for k in range(blocks)]
        return wide, extras

    def compact(j):
        wide, put_extra = placing(j, False)
        pieces = got[:, :, starts[j] : starts[j] + lanes].reshape(spread_rows, lanes)
        both = [dot(wide[b], pieces) for b in range(2)]
        extras = got[:, :, extra_at : extra_at + 128].reshape(spread_rows, 128)
        for k in range(blocks):
            value = both[k % 2][:, k // 2 * 128 : (k // 2 + 1) * 128]
            if j == 0:
                value = value + dot(put_extra[k], extras)
            at = k * 128 % lanes
            if k * 128 < lanes:
                xa[j][x, t, c, :, at : at + 128] = value.astype(BF)
            else:
                xb[j][t, x, c, :, at : at + 128] = value.astype(BF)

    half = lanes // 2

    def part_of(h):
        return pl.ds(h * half, half)

    class Gather:
        def __init__(self, view, block, me, device_of):
            self.view, self.block = view, block
            self.left, self.right, self.far = mod(me - 1, RING), mod(me + 1, RING), mod(me + 2, RING)
            self.to_left, self.to_right = device_of(self.left), device_of(self.right)
            send = lambda pos, h, to: links.send(view(pos, h), view(pos, h), to)
            self.from_left = [send(me, 0, self.to_right)]
            self.from_right = [send(me, 1, self.to_left)]
            self.from_left.append(send(me, 1, self.to_right))
            self.from_right.append(send(me, 0, self.to_left))

        def pass_on(self):
            self.from_left[0].wait_recv()
            self.pass_halves(self.from_right[0].wait_recv)

        def pass_halves(self, wait_other):
            self.far_group = links.group()
            left = self.view(self.left, 0)
            links.send(left, left, self.to_right, self.far_group)
            wait_other()
            right = self.view(self.right, 1)
            links.send(right, right, self.to_left, self.far_group)

        def wait_left(self):
            self.from_left[1].wait_recv()

        def wait_right(self):
            self.from_right[1].wait_recv()

        def wait_far(self):
            links.arrived(self.far_group, self.block(self.far), self.to_left)

    class PiecewiseGather(Gather):
        def __init__(self, view, block, piece, me, device_of, short):
            self.view, self.block, self.piece, self.me = view, block, piece, me
            self.left, self.right, self.far = mod(me - 1, RING), mod(me + 1, RING), mod(me + 2, RING)
            self.to_left, self.to_right = device_of(self.left), device_of(self.right)
            self.order = (mod(short, RING), mod(short - 1, RING), mod(short + 1, RING), mod(short + 2, RING))
            self.right_going = links.group(), links.group()
            self.left_going = links.group(), links.group()

        def feed(self, n):
            for turn in range(2):
                for h, going, to in (
                    (turn, self.right_going, self.to_right),
                    (1 - turn, self.left_going, self.to_left),
                ):
                    block = self.piece(self.me, h, self.order[n])
                    links.send(block, block, to, going[h])

        def arrived(self, going, pos, h):
            links.arrived(going[h], self.view(pos, h), self.to_left)

        def pass_on(self):
            self.arrived(self.right_going, self.left, 0)
            self.pass_halves(lambda: self.arrived(self.left_going, self.right, 1))

        def wait_left(self):
            self.arrived(self.right_going, self.left, 1)

        def wait_right(self):
            self.arrived(self.left_going, self.right, 0)

    def small_gathers(j):
        return (
            Gather(
                lambda pos, h: xa[j].at[x, pos, c, :, part_of(h)], lambda pos: xa[j].at[x, pos, c], t, y_of
            ),
            Gather(
                lambda pos, h: xb[j].at[t, pos, c, :, part_of(h)], lambda pos: xb[j].at[t, pos, c], x, x_of
            ),
        )

    def big_gathers(j):
        return (
            PiecewiseGather(
                lambda pos, h: xa[j].at[pos, :, c, :, part_of(h)],
                lambda pos: xa[j].at[pos, :, c],
                lambda pos, h, n: xa[j].at[pos, n, c, :, part_of(h)],
                x, x_of, t,
            ),
            PiecewiseGather(
                lambda pos, h: xb[j].at[pos, :, c, :, part_of(h)],
                lambda pos: xb[j].at[pos, :, c],
                lambda pos, h, n: xb[j].at[pos, n, c, :, part_of(h)],
                t, y_of, x,
            ),
        )

    def feed_own(longs):
        for long in longs:
            long.feed(0)

    def feed_sides(shorts, longs):
        for short, long in zip(shorts, longs):
            short.wait_left()
            long.feed(1)
            short.wait_right()
            long.feed(2)

    def feed_far(shorts, longs):
        for short, long in zip(shorts, longs):
            short.wait_far()
            long.feed(3)

    def pass_on(gathers):
        for gather in gathers:
            gather.pass_on()

    def share_core(buf, pos, j):
        return links.send(buf[j].at[pos, :, c], buf[j].at[pos, :, c], partner)

    def turn(n):
        @pl.loop(0, RING)
        def _(k):
            at = pl.multiple_of(n * share + k * (share // RING), 128)
            for w, turned in ((wg, turned_g), (wu, turned_u)):
                turned[pl.ds(at, share // RING), :] = w[:, pl.ds(at, share // RING)].T

    def up_rows(w, n, second):
        return w[pl.ds(pl.multiple_of(n * share + second * lanes, 128), lanes), :]

    def columns(w, n, second):
        return w[:, pl.ds(pl.multiple_of(n * share + second * lanes, 128), lanes)]

    def up_a(copy, pos, j):
        copy.wait_recv()
        tokens_in = jnp.concatenate([xa[j][pos, y].reshape(2 * rows[j], lanes) for y in range(RING)], axis=1)
        for w, acc in ((turned_g, ga[j]), (turned_u, ua[j])):
            rows_in = jnp.concatenate([up_rows(w, y, 0) for y in range(RING)], axis=0)
            acc[pos] += dot(tokens_in, rows_in)

    def up_b(copy, pos, j):
        copy.wait_recv()
        for w, acc in ((turned_g, ga[j]), (turned_u, ua[j])):
            product = dot(xb[j][pos].reshape(2 * RING * rows[j], lanes), up_rows(w, pos, 1))
            acc[...] += product.reshape(acc.shape)

    def share_sides(gathers, j):
        shared = []
        for gather, buf, unit in zip(gathers, (xa, xb), (up_a, up_b)):
            gather.wait_left()
            shared.append((unit, share_core(buf, gather.left, j), gather.left))
            gather.wait_right()
            shared.append((unit, share_core(buf, gather.right, j), gather.right))
        return shared

    def share_far(gathers, j):
        shared = []
        for gather, buf, unit in zip(gathers, (xa, xb), (up_a, up_b)):
            gather.wait_far()
            shared.append((unit, share_core(buf, gather.far, j), gather.far))
        return shared

    def run(shared, j):
        for unit, copy, pos in shared:
            unit(copy, pos, j)

    weights[0].wait()
    weights[1].wait()
    turn(0)
    turn(1)
    received(arriving[0])
    compact(0)
    small_0, big_0 = small_gathers(0), big_gathers(0)
    feed_own(big_0)
    turn(2)
    pass_on(small_0)
    received(arriving[1])
    compact(1)
    small_1 = small_gathers(1)
    feed_sides(small_0, big_0)
    feed_far(small_0, big_0)
    own_0 = [(up_a, share_core(xa, x, 0), x), (up_b, share_core(xb, t, 0), t)]
    pass_on(small_1)
    turn(3)
    run(own_0, 0)
    pass_on(big_0)
    big_1 = big_gathers(1)
    feed_own(big_1)
    feed_sides(small_1, big_1)
    feed_far(small_1, big_1)
    own_1 = [(up_a, share_core(xa, x, 1), x), (up_b, share_core(xb, t, 1), t)]
    sides_0 = share_sides(big_0, 0)
    run(own_1, 1)
    run(sides_0[:2], 0)
    far_0 = share_far(big_0, 0)
    run(sides_0[2:], 0)
    pass_on(big_1)
    run(far_0, 0)

    def activate(pos, j):
        gate = ga[j][pos]
        act[j][pos] = (gate / (1.0 + jnp.exp(-gate)) * ua[j][pos]).astype(BF)

    def down_a(pos, j):
        columns_in = jnp.concatenate([columns(wd, y, 0) for y in range(RING)], axis=1)
        product = dot(act[j][pos], columns_in).astype(BF)
        for y in range(RING):
            pa[j][pos, y] = product[:, y * lanes : (y + 1) * lanes].reshape(2, rows[j], lanes)
        return links.send(pa[j].at[pos, :, other], qa[j].at[pos], partner)

    def down_b(pos, j):
        tokens_in = act[j][...].reshape(2 * RING * rows[j], act[j].shape[2])
        product = dot(tokens_in, columns(wd, pos, 1)).astype(BF)
        pb[j][pos] = product.reshape(RING, 2, rows[j], lanes)
        return links.send(pb[j].at[pos, :, other], qb[j].at[pos], partner)

    def add_pair(copy, part, came, pos, j):
        copy.wait_recv()

        @pl.loop(0, RING)
        def _(n):
            part[j][pos, n, c] = (part[j][pos, n, c].astype(F32) + came[j][pos, n].astype(F32)).astype(BF)

    class Scatter:
        def __init__(self, view, slots, me, device_of):
            self.view, self.slots, self.me = view, slots, me
            self.left, self.right, self.far = mod(me - 1, RING), mod(me + 1, RING), mod(me + 2, RING)
            self.to_left, self.to_right = device_of(self.left), device_of(self.right)

        def send_far(self):
            self.rightward = links.send(self.view(self.far, 0), self.slots.at[0], self.to_right)
            self.leftward = links.send(self.view(self.far, 1), self.slots.at[1], self.to_left)

            self.last_group = links.group()

        def send_right(self):
            links.send(self.view(self.right, 1), self.slots.at[2], self.to_right, self.last_group)

        def send_left(self):
            links.send(self.view(self.left, 0), self.slots.at[3], self.to_left, self.last_group)

        def send_sums(self, add):
            self.rightward.wait_recv()
            add(self.right, 0, self.slots.at[0])
            links.send(self.view(self.right, 0), self.slots.at[4], self.to_right, self.last_group)
            self.leftward.wait_recv()
            add(self.left, 1, self.slots.at[1])
            links.send(self.view(self.left, 1), self.slots.at[5], self.to_left, self.last_group)

        def wait(self):
            links.arrived(self.last_group, self.slots.at[2:6], self.to_left)

        def parts(self, h):
            return (self.slots.at[4], self.slots.at[3]) if h == 0 else (self.slots.at[2], self.slots.at[5])

    def adder(part, j):
        def add(pos, h, slot):
            @pl.loop(0, RING)
            def _(n):
                own = part[j][pos, n, c, :, part_of(h)].astype(F32)
                part[j][pos, n, c, :, part_of(h)] = (own + slot[n].astype(F32)).astype(BF)

        return add

    rs_a = [Scatter(lambda pos, h, j=j: pa[j].at[pos, :, c, :, part_of(h)], ra[j], x, x_of) for j in range(2)]
    rs_b = [Scatter(lambda pos, h, j=j: pb[j].at[pos, :, c, :, part_of(h)], rb[j], t, y_of) for j in range(2)]

    def send_others(j):
        one, two = rs_a[j], rs_b[j]
        activate(one.far, j)
        pair_a = down_a(one.far, j)

        @pl.loop(1, RING)
        def _(n):
            activate(mod(one.far + n, RING), j)

        pair_b = down_b(two.far, j)
        add_pair(pair_a, pa, qa, one.far, j)
        one.send_far()
        pair_a = down_a(one.right, j)
        add_pair(pair_b, pb, qb, two.far, j)
        two.send_far()
        pair_b = down_b(two.right, j)
        add_pair(pair_a, pa, qa, one.right, j)
        one.send_right()
        pair_a = down_a(one.left, j)
        add_pair(pair_b, pb, qb, two.right, j)
        two.send_right()
        pair_b = down_b(two.left, j)
        add_pair(pair_a, pa, qa, one.left, j)
        one.send_left()
        add_pair(pair_b, pb, qb, two.left, j)
        two.send_left()

    def finish_big(scatter, part, total, me, j):
        scatter.wait()

        @pl.loop(0, RING)
        def _(n):
            for h in range(2):
                one, two = scatter.parts(h)
                value = part[j][me, n, c, :, part_of(h)].astype(F32)
                total[j][n, :, part_of(h)] = (value + one[n].astype(F32) + two[n].astype(F32)).astype(BF)

    def small_scatters(j):
        smalls = []
        for big, part, total, slots, me, to, of in (
            (rs_a[j], pa, ta, sa, x, t, y_of),
            (rs_b[j], pb, tb, sb, t, x, x_of),
        ):
            finish_big(big, part, total, me, j)
            small = Scatter(lambda pos, h, total=total: total[j].at[pos, :, part_of(h)], slots[j], to, of)
            small.send_far()
            small.send_right()
            small.send_left()
            smalls.append(small)
        return smalls

    def small_sums(smalls, j):
        for small, total in zip(smalls, (ta, tb)):

            def add(pos, h, slot):
                own = total[j][pos, :, part_of(h)].astype(F32)
                total[j][pos, :, part_of(h)] = (own + slot[...].astype(F32)).astype(BF)

            small.send_sums(add)

    def send_back(smalls, j):
        for small, total, result in zip(smalls, (ta, tb), (ea, eb)):
            small.wait()
            for h in range(2):
                one, two = small.parts(h)
                value = total[j][small.me, :, part_of(h)].astype(F32)
                value = value + one[...].astype(F32) + two[...].astype(F32)
                result[j][:, part_of(h)] = value.astype(BF)

        def block(k):
            at = k * 128 % lanes
            return (ea if k * 128 < lanes else eb)[j][:, at : at + 128]

        wide, take_extra = placing(j, True)
        picked = sum(
            dot(wide[b], jnp.concatenate([block(2 * p + b) for p in range(blocks // 2)], axis=1))
            for b in range(2)
        )
        back_sent[:, :, starts[j] : starts[j] + lanes] = picked.astype(BF).reshape(experts, MAIN, lanes)
        if j == 0:
            extra = sum(dot(take_extra[k], block(k)) for k in range(blocks))
            back_sent[:, :, extra_at : extra_at + 128] = extra.astype(BF).reshape(experts, MAIN, 128)
        return exchange(back_sent, back, starts[j], ends[j])

    def gated(j, k):
        pieces = back[:, :, starts[j] + k // 2 * 128 : starts[j] + (k // 2 + 1) * 128].reshape(spread_rows, 128)
        extras = back[:, :, extra_at : extra_at + 128].reshape(spread_rows, 128)
        value = jnp.zeros((tokens, 128), F32)
        for gate, n in ((1, 3), (2, 6)):
            picked = dot(chosen_masks(n + 2 * j, float(k % 2))[:, :spread_rows], pieces)
            if j == 0:
                picked = picked + dot(chosen_masks(n + 1, 2.0 * k)[:, :spread_rows], extras)
            value = value + keep[gate] * picked
        return value

    weights[2].wait()
    send_others(0)
    sides_1 = share_sides(big_1, 1)
    own_a, own_b = down_a(x, 0), down_b(t, 0)
    run(sides_1, 1)
    far_1 = share_far(big_1, 1)
    add_pair(own_a, pa, qa, x, 0)
    add_pair(own_b, pb, qb, t, 0)
    rs_a[0].send_sums(adder(pa, 0))
    rs_b[0].send_sums(adder(pb, 0))
    run(far_1, 1)
    send_others(1)
    own_a, own_b = down_a(x, 1), down_b(t, 1)
    last_0 = small_scatters(0)
    add_pair(own_a, pa, qa, x, 1)
    add_pair(own_b, pb, qb, t, 1)
    rs_a[1].send_sums(adder(pa, 1))
    rs_b[1].send_sums(adder(pb, 1))
    small_sums(last_0, 0)
    last_1 = small_scatters(1)
    returning = [send_back(last_0, 0)]
    small_sums(last_1, 1)
    returning.append(send_back(last_1, 1))
    received(returning[0])
    for k in range(blocks):
        mixed[:, k * 128 : (k + 1) * 128] = gated(0, k)
    received(returning[1])

    cross = jnp.zeros((tokens, 1), F32)
    squares = jnp.zeros((tokens, 1), F32)
    for k in range(blocks):
        mixture = mixed[:, k * 128 : (k + 1) * 128] + gated(1, k)
        own = h_ref[:, own_lanes(k)].astype(F32)
        output = (own + mixture).astype(BF)
        out_ref[:, k * 128 : (k + 1) * 128] = output
        output = output.astype(F32)
        cross = cross + jnp.sum(own * output, axis=1, keepdims=True)
        squares = squares + jnp.sum(output * output, axis=1, keepdims=True)

    out_copy = pltpu.make_async_copy(out_ref, out_hbm, weight_sems.at[7])
    out_copy.start()

    def total_over(buf, me, count, axis):
        group = links.group()
        for k in range(1, count):
            links.send(buf.at[me], buf.at[me], {axis: mod(me + k, count)}, group)
        links.arrived(group, buf.at[: count - 1], partner)
        total = buf[0]
        for n in range(1, count):
            total = total + buf[n]
        return total

    sums[t] = jnp.where(lane == 0, cross, jnp.where(lane == 1, squares, 0.0))
    both = total_over(sums, t, RING, "tensor")
    in_mean = keep[0][:, 0:1]
    cosine = both[:, 0:1] / width * lax.rsqrt((in_mean + EPS_COS) * (both[:, 1:2] / width + EPS_COS))
    local = jnp.sum(1.0 - cosine, axis=0, keepdims=True)
    totals[z] = jnp.broadcast_to(local, totals.shape[1:])
    grand[d] = total_over(totals, z, experts, "expert")
    score = total_over(grand, d, dp_count, "dp") / (tokens * experts * dp_count)
    score_ref[0, 0] = score[0, 0]
    out_copy.wait()
    links.drain()


def shards(hidden_in, expert_ids, ffn_gain, w_router, w_gate, w_up, w_down):
    tokens, width = hidden_in.shape[1:]
    top = expert_ids.shape[2]
    experts = lax.axis_size("expert")
    hidden = w_gate.shape[2]
    cap = max(2, 9 * tokens * top // (8 * experts))
    share = width // RING
    lanes = share // 2
    piece = (experts, MAIN, share + 128)
    hbm = pl.BlockSpec(memory_space=pl.ANY)
    scratch = lambda shape, kind: pltpu.VMEM(shape, kind)
    rows = [experts * n for n in SLOTS]
    assert sum(SLOTS) == cap
    chunked = [
        (lambda r: (RING, RING, 2, r, lanes), BF),
        (lambda r: (RING, RING, 2, r, lanes), BF),
        (lambda r: (RING, 2 * r, hidden), F32),
        (lambda r: (RING, 2 * r, hidden), F32),
        (lambda r: (RING, 2 * r, hidden), BF),
        (lambda r: (RING, RING, 2, r, lanes), BF),
        (lambda r: (RING, RING, 2, r, lanes), BF),
        (lambda r: (RING, RING, r, lanes), BF),
        (lambda r: (RING, RING, r, lanes), BF),
        (lambda r: (6, RING, r, lanes // 2), BF),
        (lambda r: (6, RING, r, lanes // 2), BF),
        (lambda r: (RING, r, lanes), BF),
        (lambda r: (RING, r, lanes), BF),
        (lambda r: (6, r, lanes // 2), BF),
        (lambda r: (6, r, lanes // 2), BF),
        (lambda r: (r, lanes), BF),
        (lambda r: (r, lanes), BF),
    ]
    out, score = pl.pallas_call(
        functools.partial(kernel, (experts, cap)),
        out_shape=(
            jax.ShapeDtypeStruct((tokens, share), BF),
            jax.ShapeDtypeStruct((1, 1), F32),
        ),
        in_specs=[hbm] * 7,
        out_specs=(hbm, pl.BlockSpec(memory_space=pltpu.SMEM)),
        scratch_shapes=[
            scratch((tokens, width), BF),
            scratch((top, tokens), jnp.int32),
            scratch((1, width), F32),
            scratch((experts, width), BF),
            scratch((tokens, share), BF),
            scratch((hidden, width), BF),
            scratch((hidden, width), BF),
            scratch((hidden, width), BF),
            scratch((width, hidden), BF),
            scratch((width, hidden), BF),
            scratch((tokens, width), BF),
            scratch((9, tokens, 128), F32),
            scratch(piece, BF),
            scratch(piece, BF),
            scratch(piece, BF),
            scratch(piece, BF),
            *[scratch(shape(r), kind) for shape, kind in chunked for r in rows],
            scratch((tokens, share), F32),
            scratch((RING, tokens, 128), F32),
            scratch((experts, 8, 128), F32),
            scratch((2 * RING, 8, 128), F32),
            pltpu.SemaphoreType.DMA((SENDS,)),
            pltpu.SemaphoreType.DMA((103,)),
            pltpu.SemaphoreType.DMA((8,)),
        ],
        compiler_params=pltpu.CompilerParams(
            collective_id=0, has_side_effects=True, vmem_limit_bytes=67043328
        ),
        name="layer",
    )(
        hidden_in.reshape(tokens, width),
        expert_ids.reshape(tokens, top).T,
        ffn_gain.reshape(1, width),
        w_router.T,
        w_gate.reshape(width, hidden).T,
        w_up.reshape(width, hidden).T,
        w_down.reshape(hidden, width),
    )
    return out.reshape(1, tokens, share), score[0, 0]


def solution(mesh):
    return jax.shard_map(
        shards,
        mesh=mesh,
        in_specs=(
            P("dp", "expert", None),
            P("dp", "expert", None),
            P(),
            P(),
            P("expert", None, ("tensor", "dp")),
            P("expert", None, ("tensor", "dp")),
            P("expert", ("tensor", "dp"), None),
        ),
        out_specs=(P("dp", "expert", "tensor"), P()),
        check_vma=False,
    )
```

```python
import functools

import jax
import jax.numpy as jnp
from jax import lax
from jax.experimental import pallas as pl
from jax.experimental.pallas import tpu as pltpu
from jax.sharding import PartitionSpec as P

EPS_NORM = 1e-05
EPS_COS = 1e-06
BF = jnp.bfloat16
F32 = jnp.float32
RING = 4
SENDS = 40
MAIN = 16
SLOTS = (10, 8)
WIDE = 8


class Links:
    def __init__(self, send_sems, recv_sems):
        self.send_sems, self.recv_sems, self.groups, self.started = send_sems, recv_sems, 0, []

    def group(self):
        self.groups += 1
        return self.groups - 1

    def send(self, src, dst, device, group=None):
        n = len(self.started)
        if n >= SENDS:
            self.started[n - SENDS].wait_send()
        copy = pltpu.make_async_remote_copy(
            src_ref=src,
            dst_ref=dst,
            send_sem=self.send_sems.at[n % SENDS],
            recv_sem=self.recv_sems.at[self.group() if group is None else group],
            device_id=device,
            device_id_type=pl.DeviceIdType.MESH,
        )
        copy.start()
        self.started.append(copy)
        return copy

    def arrived(self, group, whole, device):
        pltpu.make_async_remote_copy(
            src_ref=whole,
            dst_ref=whole,
            send_sem=self.send_sems.at[0],
            recv_sem=self.recv_sems.at[group],
            device_id=device,
            device_id_type=pl.DeviceIdType.MESH,
        ).wait_recv()

    def drain(self):
        for copy in self.started[-SENDS:]:
            copy.wait_send()


def mod(value, n):
    return lax.rem(value + 2 * n, n)


def dot(a, b):
    return jnp.dot(a, b, preferred_element_type=F32)


def dot_rows(a, b):
    return lax.dot_general(a, b, (((1,), (1,)), ((), ())), preferred_element_type=F32)


def onehot(mask):
    return jnp.where(mask, 1.0, 0.0).astype(BF)


def kernel(
    sizes,
    h_hbm, ids_hbm, gain_hbm, router_hbm, wg_hbm, wu_hbm, wd_hbm,
    out_hbm, score_ref,
    h_ref, ids_ref, gain_ref, router_ref, out_ref,
    wg, wu, wd, turned_g, turned_u, normed, keep, sent, got, back_sent, back,
    *buffers,
):
    *buffers, mixed, sums, totals, grand, send_sems, recv_sems, weight_sems = buffers
    xa, xb, ga, ua, act, pa, pb, qa, qb, ra, rb, ta, tb, sa, sb, ea, eb = zip(buffers[::2], buffers[1::2])
    experts, cap = sizes
    tokens, width = h_hbm.shape
    share = width // RING
    lanes = share // 2
    rows = [experts * n for n in SLOTS]
    spread_rows = experts * MAIN
    blocks = share // 128
    z = lax.axis_index("expert")
    t = lax.axis_index("tensor")
    d = lax.axis_index("dp")
    x, c = d // 2, lax.rem(d, 2)
    other = 1 - c
    x_of = lambda pos: {"dp": pos * 2 + c}
    y_of = lambda pos: {"tensor": pos}
    partner = {"dp": x * 2 + other}
    dp_count = RING * 2

    barrier = pltpu.get_barrier_semaphore()
    peers = (
        [{"expert": mod(z + k, experts)} for k in range(1, experts)]
        + [{"tensor": mod(t + k, RING)} for k in range(1, RING)]
        + [{"dp": mod(d + k, dp_count)} for k in range(1, dp_count)]
    )
    for peer in peers:
        pl.semaphore_signal(barrier, inc=1, device_id=peer, device_id_type=pl.DeviceIdType.MESH)

    weights = [
        pltpu.make_async_copy(src, dst, weight_sems.at[n])
        for n, (src, dst) in enumerate(
            (
                (wg_hbm, wg), (wu_hbm, wu), (wd_hbm, wd),
                (h_hbm, h_ref), (ids_hbm, ids_ref), (gain_hbm, gain_ref), (router_hbm, router_ref),
            )
        )
    ]
    for copy in weights[3:] + weights[:3]:
        copy.start()
    for copy in weights[3:]:
        copy.wait()

    token_rows = h_ref[...].astype(F32)
    in_squares = jnp.sum(token_rows * token_rows, axis=1, keepdims=True) / width
    normed[...] = (token_rows * lax.rsqrt(in_squares + EPS_NORM) * gain_ref[...]).astype(BF)
    logits = dot_rows(normed[...], router_ref[...])
    lane = lax.broadcasted_iota(jnp.int32, (tokens, 128), 1)
    lane_f = lane.astype(F32)
    ids = ids_ref[...].astype(F32)
    row_of = lax.broadcasted_iota(jnp.int32, (tokens, tokens), 0)
    lane_of = lax.broadcasted_iota(jnp.int32, (tokens, tokens), 1)
    first_f, second_f = (
        jnp.sum(jnp.where(row_of == lane_of, ids[n : n + 1], 0.0), axis=1, keepdims=True) for n in range(2)
    )
    is_first = jnp.where(lane_f == first_f, 1.0, 0.0)
    is_second = jnp.where(lane_f == second_f, 1.0, 0.0)
    spread = jnp.sum((is_first[:, :experts] - is_second[:, :experts]) * logits, axis=1, keepdims=True)
    gate_first = 1.0 / (1.0 + jnp.exp(-spread))
    gate_second = 1.0 / (1.0 + jnp.exp(spread))
    before = dot(onehot(lane_of < row_of), (is_first + is_second).astype(BF))
    kept = [in_squares, gate_first, gate_second]
    for chosen, mask in ((first_f, is_first), (second_f, is_second)):
        slot = jnp.sum(before * mask, axis=1, keepdims=True)
        place = chosen * MAIN
        late = slot - SLOTS[0]
        kept.append(jnp.where(slot < WIDE, place + 2.0 * slot, -1000.0))
        kept.append(jnp.where((slot >= WIDE) & (late < 0.0), place + slot - WIDE, -1000.0))
        kept.append(jnp.where(late >= 0.0, place + 2.0 * late, -1000.0))
    for n, column in enumerate(kept):
        keep[n] = jnp.broadcast_to(column, (tokens, 128))

    def chosen_masks(n, shift):
        return onehot(lane_f - shift == keep[n])

    extra_at = lanes
    starts, ends = (0, lanes + 128), (lanes + 128, 2 * lanes + 128)

    def picks(n, shift):
        return (chosen_masks(n, shift) + chosen_masks(n + 3, shift)).astype(F32).T.astype(BF)[:spread_rows]

    def own_lanes(k):
        return pl.ds(pl.multiple_of(t * share + k * 128, 128), 128)

    for j in range(2):
        select = [picks(3 + 2 * j, float(b)) for b in range(2)]
        for p in range(blocks // 2):
            picked = sum(dot(select[b], normed[:, own_lanes(2 * p + b)]) for b in range(2))
            at = starts[j] + p * 128
            sent[:, :, at : at + 128] = picked.astype(BF).reshape(experts, MAIN, 128)
    extra = sum(dot(picks(4, 2.0 * k), normed[:, own_lanes(k)]) for k in range(blocks))
    sent[:, :, extra_at : extra_at + 128] = extra.astype(BF).reshape(experts, MAIN, 128)

    for acc in ga + ua:
        acc[...] = jnp.zeros_like(acc)
    pl.semaphore_wait(barrier, len(peers))
    links = Links(send_sems, recv_sems)

    def exchange(src, dst, begin, end):
        group = links.group()
        for k in sorted(range(1, experts), key=lambda k: -min(k, experts - k)):
            to = mod(z + k, experts)
            links.send(src.at[to, :, begin:end], dst.at[z, :, begin:end], {"expert": to}, group)
        dst[z, :, begin:end] = src[z, :, begin:end]
        return group, dst.at[: experts - 1, :, begin:end]

    def received(exchanged):
        links.arrived(*exchanged, partner)

    arriving = [exchange(sent, got, starts[j], ends[j]) for j in range(2)]

    def placing(j, transposed):
        shape = (spread_rows, rows[j]) if transposed else (rows[j], spread_rows)
        row = lax.broadcasted_iota(jnp.int32, shape, 1 if transposed else 0)
        place = lax.broadcasted_iota(jnp.int32, shape, 0 if transposed else 1)
        base, within = place // MAIN * SLOTS[j], place % MAIN
        wide = [onehot((row == base + within // 2) & (within % 2 == b)) for b in range(2)]
        extras = [onehot((row == base + WIDE + within % 2) & (within // 2 == k)) for k in range(blocks)]
        return wide, extras

    def compact(j):
        wide, put_extra = placing(j, False)
        pieces = got[:, :, starts[j] : starts[j] + lanes].reshape(spread_rows, lanes)
        both = [dot(wide[b], pieces) for b in range(2)]
        extras = got[:, :, extra_at : extra_at + 128].reshape(spread_rows, 128)
        for k in range(blocks):
            value = both[k % 2][:, k // 2 * 128 : (k // 2 + 1) * 128]
            if j == 0:
                value = value + dot(put_extra[k], extras)
            at = k * 128 % lanes
            if k * 128 < lanes:
                xa[j][x, t, c, :, at : at + 128] = value.astype(BF)
            else:
                xb[j][t, x, c, :, at : at + 128] = value.astype(BF)

    half = lanes // 2

    def part_of(h):
        return pl.ds(h * half, half)

    class Gather:
        def __init__(self, view, block, me, device_of):
            self.view, self.block = view, block
            self.left, self.right, self.far = mod(me - 1, RING), mod(me + 1, RING), mod(me + 2, RING)
            self.to_left, self.to_right = device_of(self.left), device_of(self.right)
            send = lambda pos, h, to: links.send(view(pos, h), view(pos, h), to)
            self.from_left = [send(me, 0, self.to_right)]
            self.from_right = [send(me, 1, self.to_left)]
            self.from_left.append(send(me, 1, self.to_right))
            self.from_right.append(send(me, 0, self.to_left))

        def pass_on(self):
            self.from_left[0].wait_recv()
            self.pass_halves(self.from_right[0].wait_recv)

        def pass_halves(self, wait_other):
            self.far_group = links.group()
            left = self.view(self.left, 0)
            links.send(left, left, self.to_right, self.far_group)
            wait_other()
            right = self.view(self.right, 1)
            links.send(right, right, self.to_left, self.far_group)

        def wait_left(self):
            self.from_left[1].wait_recv()

        def wait_right(self):
            self.from_right[1].wait_recv()

        def wait_far(self):
            links.arrived(self.far_group, self.block(self.far), self.to_left)

    class PiecewiseGather(Gather):
        def __init__(self, view, block, piece, me, device_of, short):
            self.view, self.block, self.piece, self.me = view, block, piece, me
            self.left, self.right, self.far = mod(me - 1, RING), mod(me + 1, RING), mod(me + 2, RING)
            self.to_left, self.to_right = device_of(self.left), device_of(self.right)
            self.order = (mod(short, RING), mod(short - 1, RING), mod(short + 1, RING), mod(short + 2, RING))
            self.right_going = links.group(), links.group()
            self.left_going = links.group(), links.group()

        def feed(self, n):
            for turn in range(2):
                for h, going, to in (
                    (turn, self.right_going, self.to_right),
                    (1 - turn, self.left_going, self.to_left),
                ):
                    block = self.piece(self.me, h, self.order[n])
                    links.send(block, block, to, going[h])

        def arrived(self, going, pos, h):
            links.arrived(going[h], self.view(pos, h), self.to_left)

        def pass_on(self):
            self.arrived(self.right_going, self.left, 0)
            self.pass_halves(lambda: self.arrived(self.left_going, self.right, 1))

        def wait_left(self):
            self.arrived(self.right_going, self.left, 1)

        def wait_right(self):
            self.arrived(self.left_going, self.right, 0)

    def small_gathers(j):
        return (
            Gather(
                lambda pos, h: xa[j].at[x, pos, c, :, part_of(h)], lambda pos: xa[j].at[x, pos, c], t, y_of
            ),
            Gather(
                lambda pos, h: xb[j].at[t, pos, c, :, part_of(h)], lambda pos: xb[j].at[t, pos, c], x, x_of
            ),
        )

    def big_gathers(j):
        return (
            PiecewiseGather(
                lambda pos, h: xa[j].at[pos, :, c, :, part_of(h)],
                lambda pos: xa[j].at[pos, :, c],
                lambda pos, h, n: xa[j].at[pos, n, c, :, part_of(h)],
                x, x_of, t,
            ),
            PiecewiseGather(
                lambda pos, h: xb[j].at[pos, :, c, :, part_of(h)],
                lambda pos: xb[j].at[pos, :, c],
                lambda pos, h, n: xb[j].at[pos, n, c, :, part_of(h)],
                t, y_of, x,
            ),
        )

    def feed_own(longs):
        for long in longs:
            long.feed(0)

    def feed_sides(shorts, longs):
        for short, long in zip(shorts, longs):
            short.wait_left()
            long.feed(1)
            short.wait_right()
            long.feed(2)

    def feed_far(shorts, longs):
        for short, long in zip(shorts, longs):
            short.wait_far()
            long.feed(3)

    def pass_on(gathers):
        for gather in gathers:
            gather.pass_on()

    def share_core(buf, pos, j):
        return links.send(buf[j].at[pos, :, c], buf[j].at[pos, :, c], partner)

    def turn(n):
        @pl.loop(0, RING)
        def _(k):
            at = pl.multiple_of(n * share + k * (share // RING), 128)
            for w, turned in ((wg, turned_g), (wu, turned_u)):
                turned[pl.ds(at, share // RING), :] = w[:, pl.ds(at, share // RING)].T

    def up_rows(w, n, second):
        return w[pl.ds(pl.multiple_of(n * share + second * lanes, 128), lanes), :]

    def columns(w, n, second):
        return w[:, pl.ds(pl.multiple_of(n * share + second * lanes, 128), lanes)]

    def up_a(copy, pos, j):
        copy.wait_recv()
        tokens_in = jnp.concatenate([xa[j][pos, y].reshape(2 * rows[j], lanes) for y in range(RING)], axis=1)
        for w, acc in ((turned_g, ga[j]), (turned_u, ua[j])):
            rows_in = jnp.concatenate([up_rows(w, y, 0) for y in range(RING)], axis=0)
            acc[pos] += dot(tokens_in, rows_in)

    def up_b(copy, pos, j):
        copy.wait_recv()
        for w, acc in ((turned_g, ga[j]), (turned_u, ua[j])):
            product = dot(xb[j][pos].reshape(2 * RING * rows[j], lanes), up_rows(w, pos, 1))
            acc[...] += product.reshape(acc.shape)

    def share_sides(gathers, j):
        shared = []
        for gather, buf, unit in zip(gathers, (xa, xb), (up_a, up_b)):
            gather.wait_left()
            shared.append((unit, share_core(buf, gather.left, j), gather.left))
            gather.wait_right()
            shared.append((unit, share_core(buf, gather.right, j), gather.right))
        return shared

    def share_far(gathers, j):
        shared = []
        for gather, buf, unit in zip(gathers, (xa, xb), (up_a, up_b)):
            gather.wait_far()
            shared.append((unit, share_core(buf, gather.far, j), gather.far))
        return shared

    def run(shared, j):
        for unit, copy, pos in shared:
            unit(copy, pos, j)

    weights[0].wait()
    weights[1].wait()
    turn(0)
    turn(1)
    received(arriving[0])
    compact(0)
    small_0, big_0 = small_gathers(0), big_gathers(0)
    feed_own(big_0)
    turn(2)
    pass_on(small_0)
    received(arriving[1])
    compact(1)
    small_1 = small_gathers(1)
    feed_sides(small_0, big_0)
    feed_far(small_0, big_0)
    own_0 = [(up_a, share_core(xa, x, 0), x), (up_b, share_core(xb, t, 0), t)]
    pass_on(small_1)
    turn(3)
    run(own_0, 0)
    pass_on(big_0)
    big_1 = big_gathers(1)
    feed_own(big_1)
    feed_sides(small_1, big_1)
    feed_far(small_1, big_1)
    own_1 = [(up_a, share_core(xa, x, 1), x), (up_b, share_core(xb, t, 1), t)]
    sides_0 = share_sides(big_0, 0)
    run(own_1, 1)
    run(sides_0[:2], 0)
    far_0 = share_far(big_0, 0)
    run(sides_0[2:], 0)
    pass_on(big_1)
    run(far_0, 0)

    def activate(pos, j):
        gate = ga[j][pos]
        act[j][pos] = (gate / (1.0 + jnp.exp(-gate)) * ua[j][pos]).astype(BF)

    def down_a(pos, j):
        columns_in = jnp.concatenate([columns(wd, y, 0) for y in range(RING)], axis=1)
        product = dot(act[j][pos], columns_in).astype(BF)
        for y in range(RING):
            pa[j][pos, y] = product[:, y * lanes : (y + 1) * lanes].reshape(2, rows[j], lanes)
        return links.send(pa[j].at[pos, :, other], qa[j].at[pos], partner)

    def down_b(pos, j):
        tokens_in = act[j][...].reshape(2 * RING * rows[j], act[j].shape[2])
        product = dot(tokens_in, columns(wd, pos, 1)).astype(BF)
        pb[j][pos] = product.reshape(RING, 2, rows[j], lanes)
        return links.send(pb[j].at[pos, :, other], qb[j].at[pos], partner)

    def add_pair(copy, part, came, pos, j):
        copy.wait_recv()

        @pl.loop(0, RING)
        def _(n):
            part[j][pos, n, c] = (part[j][pos, n, c].astype(F32) + came[j][pos, n].astype(F32)).astype(BF)

    class Scatter:
        def __init__(self, view, slots, me, device_of):
            self.view, self.slots, self.me = view, slots, me
            self.left, self.right, self.far = mod(me - 1, RING), mod(me + 1, RING), mod(me + 2, RING)
            self.to_left, self.to_right = device_of(self.left), device_of(self.right)

        def send_far(self):
            self.rightward = links.send(self.view(self.far, 0), self.slots.at[0], self.to_right)
            self.leftward = links.send(self.view(self.far, 1), self.slots.at[1], self.to_left)

            self.last_group = links.group()

        def send_right(self):
            links.send(self.view(self.right, 1), self.slots.at[2], self.to_right, self.last_group)

        def send_left(self):
            links.send(self.view(self.left, 0), self.slots.at[3], self.to_left, self.last_group)

        def send_sums(self, add):
            self.rightward.wait_recv()
            add(self.right, 0, self.slots.at[0])
            links.send(self.view(self.right, 0), self.slots.at[4], self.to_right, self.last_group)
            self.leftward.wait_recv()
            add(self.left, 1, self.slots.at[1])
            links.send(self.view(self.left, 1), self.slots.at[5], self.to_left, self.last_group)

        def wait(self):
            links.arrived(self.last_group, self.slots.at[2:6], self.to_left)

        def parts(self, h):
            return (self.slots.at[4], self.slots.at[3]) if h == 0 else (self.slots.at[2], self.slots.at[5])

    def adder(part, j):
        def add(pos, h, slot):
            @pl.loop(0, RING)
            def _(n):
                own = part[j][pos, n, c, :, part_of(h)].astype(F32)
                part[j][pos, n, c, :, part_of(h)] = (own + slot[n].astype(F32)).astype(BF)

        return add

    rs_a = [Scatter(lambda pos, h, j=j: pa[j].at[pos, :, c, :, part_of(h)], ra[j], x, x_of) for j in range(2)]
    rs_b = [Scatter(lambda pos, h, j=j: pb[j].at[pos, :, c, :, part_of(h)], rb[j], t, y_of) for j in range(2)]

    def send_others(j):
        one, two = rs_a[j], rs_b[j]
        activate(one.far, j)
        pair_a = down_a(one.far, j)

        @pl.loop(1, RING)
        def _(n):
            activate(mod(one.far + n, RING), j)

        pair_b = down_b(two.far, j)
        add_pair(pair_a, pa, qa, one.far, j)
        one.send_far()
        pair_a = down_a(one.right, j)
        add_pair(pair_b, pb, qb, two.far, j)
        two.send_far()
        pair_b = down_b(two.right, j)
        add_pair(pair_a, pa, qa, one.right, j)
        one.send_right()
        pair_a = down_a(one.left, j)
        add_pair(pair_b, pb, qb, two.right, j)
        two.send_right()
        pair_b = down_b(two.left, j)
        add_pair(pair_a, pa, qa, one.left, j)
        one.send_left()
        add_pair(pair_b, pb, qb, two.left, j)
        two.send_left()

    def finish_big(scatter, part, total, me, j):
        scatter.wait()

        @pl.loop(0, RING)
        def _(n):
            for h in range(2):
                one, two = scatter.parts(h)
                value = part[j][me, n, c, :, part_of(h)].astype(F32)
                total[j][n, :, part_of(h)] = (value + one[n].astype(F32) + two[n].astype(F32)).astype(BF)

    def small_scatters(j):
        smalls = []
        for big, part, total, slots, me, to, of in (
            (rs_a[j], pa, ta, sa, x, t, y_of),
            (rs_b[j], pb, tb, sb, t, x, x_of),
        ):
            finish_big(big, part, total, me, j)
            small = Scatter(lambda pos, h, total=total: total[j].at[pos, :, part_of(h)], slots[j], to, of)
            small.send_far()
            small.send_right()
            small.send_left()
            smalls.append(small)
        return smalls

    def small_sums(smalls, j):
        for small, total in zip(smalls, (ta, tb)):

            def add(pos, h, slot):
                own = total[j][pos, :, part_of(h)].astype(F32)
                total[j][pos, :, part_of(h)] = (own + slot[...].astype(F32)).astype(BF)

            small.send_sums(add)

    def send_back(smalls, j):
        for small, total, result in zip(smalls, (ta, tb), (ea, eb)):
            small.wait()
            for h in range(2):
                one, two = small.parts(h)
                value = total[j][small.me, :, part_of(h)].astype(F32)
                value = value + one[...].astype(F32) + two[...].astype(F32)
                result[j][:, part_of(h)] = value.astype(BF)

        def block(k):
            at = k * 128 % lanes
            return (ea if k * 128 < lanes else eb)[j][:, at : at + 128]

        wide, take_extra = placing(j, True)
        picked = sum(
            dot(wide[b], jnp.concatenate([block(2 * p + b) for p in range(blocks // 2)], axis=1))
            for b in range(2)
        )
        back_sent[:, :, starts[j] : starts[j] + lanes] = picked.astype(BF).reshape(experts, MAIN, lanes)
        if j == 0:
            extra = sum(dot(take_extra[k], block(k)) for k in range(blocks))
            back_sent[:, :, extra_at : extra_at + 128] = extra.astype(BF).reshape(experts, MAIN, 128)
        return exchange(back_sent, back, starts[j], ends[j])

    def gated(j, k):
        pieces = back[:, :, starts[j] + k // 2 * 128 : starts[j] + (k // 2 + 1) * 128].reshape(spread_rows, 128)
        extras = back[:, :, extra_at : extra_at + 128].reshape(spread_rows, 128)
        value = jnp.zeros((tokens, 128), F32)
        for gate, n in ((1, 3), (2, 6)):
            picked = dot(chosen_masks(n + 2 * j, float(k % 2))[:, :spread_rows], pieces)
            if j == 0:
                picked = picked + dot(chosen_masks(n + 1, 2.0 * k)[:, :spread_rows], extras)
            value = value + keep[gate] * picked
        return value

    weights[2].wait()
    send_others(0)
    sides_1 = share_sides(big_1, 1)
    own_a, own_b = down_a(x, 0), down_b(t, 0)
    run(sides_1, 1)
    far_1 = share_far(big_1, 1)
    add_pair(own_a, pa, qa, x, 0)
    add_pair(own_b, pb, qb, t, 0)
    rs_a[0].send_sums(adder(pa, 0))
    rs_b[0].send_sums(adder(pb, 0))
    run(far_1, 1)
    send_others(1)
    own_a, own_b = down_a(x, 1), down_b(t, 1)
    last_0 = small_scatters(0)
    add_pair(own_a, pa, qa, x, 1)
    add_pair(own_b, pb, qb, t, 1)
    rs_a[1].send_sums(adder(pa, 1))
    rs_b[1].send_sums(adder(pb, 1))
    small_sums(last_0, 0)
    last_1 = small_scatters(1)
    returning = [send_back(last_0, 0)]
    small_sums(last_1, 1)
    returning.append(send_back(last_1, 1))
    received(returning[0])
    for k in range(blocks):
        mixed[:, k * 128 : (k + 1) * 128] = gated(0, k)
    received(returning[1])

    cross = jnp.zeros((tokens, 1), F32)
    squares = jnp.zeros((tokens, 1), F32)
    for k in range(blocks):
        mixture = mixed[:, k * 128 : (k + 1) * 128] + gated(1, k)
        own = h_ref[:, own_lanes(k)].astype(F32)
        output = (own + mixture).astype(BF)
        out_ref[:, k * 128 : (k + 1) * 128] = output
        output = output.astype(F32)
        cross = cross + jnp.sum(own * output, axis=1, keepdims=True)
        squares = squares + jnp.sum(output * output, axis=1, keepdims=True)

    out_copy = pltpu.make_async_copy(out_ref, out_hbm, weight_sems.at[7])
    out_copy.start()

    def total_over(buf, me, count, axis):
        group = links.group()
        for k in range(1, count):
            links.send(buf.at[me], buf.at[me], {axis: mod(me + k, count)}, group)
        links.arrived(group, buf.at[: count - 1], partner)
        total = buf[0]
        for n in range(1, count):
            total = total + buf[n]
        return total

    sums[t] = jnp.where(lane == 0, cross, jnp.where(lane == 1, squares, 0.0))
    both = total_over(sums, t, RING, "tensor")
    in_mean = keep[0][:, 0:1]
    cosine = both[:, 0:1] / width * lax.rsqrt((in_mean + EPS_COS) * (both[:, 1:2] / width + EPS_COS))
    local = jnp.sum(1.0 - cosine, axis=0, keepdims=True)
    totals[z] = jnp.broadcast_to(local, totals.shape[1:])
    grand[d] = total_over(totals, z, experts, "expert")
    score = total_over(grand, d, dp_count, "dp") / (tokens * experts * dp_count)
    score_ref[0, 0] = score[0, 0]
    out_copy.wait()
    links.drain()


def shards(hidden_in, expert_ids, ffn_gain, w_router, w_gate, w_up, w_down):
    tokens, width = hidden_in.shape[1:]
    top = expert_ids.shape[2]
    experts = lax.axis_size("expert")
    hidden = w_gate.shape[2]
    cap = max(2, 9 * tokens * top // (8 * experts))
    share = width // RING
    lanes = share // 2
    piece = (experts, MAIN, share + 128)
    hbm = pl.BlockSpec(memory_space=pl.ANY)
    scratch = lambda shape, kind: pltpu.VMEM(shape, kind)
    rows = [experts * n for n in SLOTS]
    assert sum(SLOTS) == cap
    chunked = [
        (lambda r: (RING, RING, 2, r, lanes), BF),
        (lambda r: (RING, RING, 2, r, lanes), BF),
        (lambda r: (RING, 2 * r, hidden), F32),
        (lambda r: (RING, 2 * r, hidden), F32),
        (lambda r: (RING, 2 * r, hidden), BF),
        (lambda r: (RING, RING, 2, r, lanes), BF),
        (lambda r: (RING, RING, 2, r, lanes), BF),
        (lambda r: (RING, RING, r, lanes), BF),
        (lambda r: (RING, RING, r, lanes), BF),
        (lambda r: (6, RING, r, lanes // 2), BF),
        (lambda r: (6, RING, r, lanes // 2), BF),
        (lambda r: (RING, r, lanes), BF),
        (lambda r: (RING, r, lanes), BF),
        (lambda r: (6, r, lanes // 2), BF),
        (lambda r: (6, r, lanes // 2), BF),
        (lambda r: (r, lanes), BF),
        (lambda r: (r, lanes), BF),
    ]
    out, score = pl.pallas_call(
        functools.partial(kernel, (experts, cap)),
        out_shape=(
            jax.ShapeDtypeStruct((tokens, share), BF),
            jax.ShapeDtypeStruct((1, 1), F32),
        ),
        in_specs=[hbm] * 7,
        out_specs=(hbm, pl.BlockSpec(memory_space=pltpu.SMEM)),
        scratch_shapes=[
            scratch((tokens, width), BF),
            scratch((top, tokens), jnp.int32),
            scratch((1, width), F32),
            scratch((experts, width), BF),
            scratch((tokens, share), BF),
            scratch((hidden, width), BF),
            scratch((hidden, width), BF),
            scratch((hidden, width), BF),
            scratch((width, hidden), BF),
            scratch((width, hidden), BF),
            scratch((tokens, width), BF),
            scratch((9, tokens, 128), F32),
            scratch(piece, BF),
            scratch(piece, BF),
            scratch(piece, BF),
            scratch(piece, BF),
            *[scratch(shape(r), kind) for shape, kind in chunked for r in rows],
            scratch((tokens, share), F32),
            scratch((RING, tokens, 128), F32),
            scratch((experts, 8, 128), F32),
            scratch((2 * RING, 8, 128), F32),
            pltpu.SemaphoreType.DMA((SENDS,)),
            pltpu.SemaphoreType.DMA((103,)),
            pltpu.SemaphoreType.DMA((8,)),
        ],
        compiler_params=pltpu.CompilerParams(
            collective_id=0, has_side_effects=True, vmem_limit_bytes=67043328
        ),
        name="layer",
    )(
        hidden_in.reshape(tokens, width),
        expert_ids.reshape(tokens, top).T,
        ffn_gain.reshape(1, width),
        w_router.T,
        w_gate.reshape(width, hidden).T,
        w_up.reshape(width, hidden).T,
        w_down.reshape(hidden, width),
    )
    return out.reshape(1, tokens, share), score[0, 0]


def solution(mesh):
    return jax.shard_map(
        shards,
        mesh=mesh,
        in_specs=(
            P("dp", "expert", None),
            P("dp", "expert", None),
            P(),
            P(),
            P("expert", None, ("tensor", "dp")),
            P("expert", None, ("tensor", "dp")),
            P("expert", ("tensor", "dp"), None),
        ),
        out_specs=(P("dp", "expert", "tensor"), P()),
        check_vma=False,
    )
```
